32 devices in a mesh: dp: 1 (over z), ep: 32 (over y, x, core).
Axes of the slice: x: 4, y: 4, z: 1, core: 2. Of those that a mesh axis runs over, the one named last changes fastest.
The devices are a block of a 4x4x8 slice.
Arguments:
- dispatched: bfloat16 [32, 128, 16, 2048], P('dp', 'ep')
- w_gate: bfloat16 [128, 2048, 768], P('ep')
- w_up: bfloat16 [128, 2048, 768], P('ep')
- w_down: bfloat16 [128, 768, 2048], P('ep')
- fill_count: int32 [32, 128], P('dp', 'ep')
- slot_index: int32 [4096, 8], P(('dp', 'ep'))
- expert_id: int32 [4096, 8], P(('dp', 'ep'))
- gate_weight: float32 [4096, 8], P(('dp', 'ep'))
Outputs:
- output: bfloat16 [4096, 2048], P(('dp', 'ep'))
All inputs are finite; a program needn't handle non-finite values.
Results may differ from the reference program's by a relative error of at most 0.00111.
Values are sent between devices in bfloat16 or wider.
A program may use at most 768 MiB of HBM per device.

```python
import jax
import jax.numpy as jnp
from jax import lax

HIDDEN = 2048
FFN_DIM = 768
EXPERTS = 128
TOP_K = 8
TOKENS_DEV = 128
GROUP_SIZE = 32
CAPACITY = (2 * TOKENS_DEV * TOP_K) // EXPERTS


def draw_routing(route_key):
    key_perm, key_noise, key_shift = jax.random.split(route_key, 3)
    popularity = jax.random.permutation(key_perm, EXPERTS)
    base_score = 4000 // (popularity + 1)
    noise_term = jax.random.randint(key_noise, (GROUP_SIZE, TOKENS_DEV, EXPERTS), 0, 1000)
    cover_shift = jax.random.randint(key_shift, (GROUP_SIZE, 1), 0, EXPERTS)
    expert_ids = jnp.arange(EXPERTS, dtype=jnp.int32)
    cover_id = (jnp.arange(TOKENS_DEV, dtype=jnp.int32)[None, :] + cover_shift) % EXPERTS
    cover_bonus = jnp.where(expert_ids[None, None, :] == cover_id[:, :, None], 100000, 0)
    route_score = (base_score[None, None, :] + noise_term + cover_bonus) * EXPERTS + expert_ids
    chosen = lax.top_k(route_score, TOP_K)[1]
    onehot = (chosen.reshape(GROUP_SIZE, TOKENS_DEV * TOP_K, 1) == expert_ids).astype(jnp.int32)
    earlier = jnp.cumsum(onehot, axis=1) - onehot
    arrival = jnp.sum(earlier * onehot, axis=2)
    slot_index = jnp.where(arrival < CAPACITY, arrival, -1)
    filled_count = jnp.minimum(jnp.sum(onehot, axis=1), CAPACITY)
    expert_id = chosen.reshape(GROUP_SIZE * TOKENS_DEV, TOP_K).astype(jnp.int32)
    slot_index = slot_index.reshape(GROUP_SIZE * TOKENS_DEV, TOP_K).astype(jnp.int32)
    return expert_id, slot_index, filled_count.astype(jnp.int32)


def setup_inputs(seed: int = 0, part: int = 0) -> dict:
    shared_key, part_root = jax.random.split(jax.random.key(seed))
    key_gate_w, key_up_w, key_down_w = jax.random.split(shared_key, 3)
    part_key = jax.random.fold_in(part_root, part)
    key_route, key_rows, key_mix = jax.random.split(part_key, 3)
    expert_id, slot_index, filled_count = draw_routing(key_route)
    dispatched = jax.random.normal(key_rows, (GROUP_SIZE, EXPERTS, CAPACITY, HIDDEN), jnp.float32)
    w_gate = jax.random.normal(key_gate_w, (EXPERTS, HIDDEN, FFN_DIM), jnp.float32) * HIDDEN ** -0.5
    w_up = jax.random.normal(key_up_w, (EXPERTS, HIDDEN, FFN_DIM), jnp.float32) * HIDDEN ** -0.5
    w_down = jax.random.normal(key_down_w, (EXPERTS, FFN_DIM, HIDDEN), jnp.float32) * FFN_DIM ** -0.5
    logits = jax.random.normal(key_mix, (GROUP_SIZE * TOKENS_DEV, TOP_K), jnp.float32) * 1.5
    return {
        "dispatched": dispatched.astype(jnp.bfloat16),
        "w_gate": w_gate.astype(jnp.bfloat16),
        "w_up": w_up.astype(jnp.bfloat16),
        "w_down": w_down.astype(jnp.bfloat16),
        "fill_count": filled_count,
        "slot_index": slot_index,
        "expert_id": expert_id,
        "gate_weight": jax.nn.softmax(logits, axis=-1),
    }


def reference(dispatched, w_gate, w_up, w_down, fill_count, slot_index, expert_id, gate_weight):
    group_size = dispatched.shape[0]
    capacity = dispatched.shape[2]
    tokens_dev = slot_index.shape[0] // group_size

    def expert_ffn(operands):
        row_block, gate_w, up_w, down_w, filled = operands
        rows_f32 = row_block.astype(jnp.float32)
        pre_gate = jnp.einsum("scd,df->scf", rows_f32, gate_w.astype(jnp.float32))
        pre_up = jnp.einsum("scd,df->scf", rows_f32, up_w.astype(jnp.float32))
        hidden = (jax.nn.silu(pre_gate) * pre_up).astype(jnp.bfloat16)
        result = jnp.einsum("scf,fd->scd", hidden.astype(jnp.float32), down_w.astype(jnp.float32)).astype(jnp.bfloat16)
        live_mask = jnp.arange(capacity)[None, :] < filled[:, None]
        return jnp.where(live_mask[:, :, None], result, jnp.zeros_like(result))

    expert_out = lax.map(expert_ffn, (jnp.swapaxes(dispatched, 0, 1), w_gate, w_up, w_down, jnp.swapaxes(fill_count, 0, 1)))
    flat_rows = expert_out.reshape(-1, expert_out.shape[-1])
    source = (jnp.arange(slot_index.shape[0]) // tokens_dev)[:, None]
    row_index = (expert_id * group_size + source) * capacity + jnp.maximum(slot_index, 0)
    weight = jnp.where(slot_index >= 0, gate_weight, 0.0)
    combined = jnp.zeros((slot_index.shape[0], flat_rows.shape[1]), jnp.float32)
    for choice in range(slot_index.shape[1]):
        picked = jnp.take(flat_rows, row_index[:, choice], axis=0).astype(jnp.float32)
        combined = combined + weight[:, choice, None] * picked
    return combined.astype(jnp.bfloat16)
```

```python
import functools

import jax
import jax.numpy as jnp
from jax import lax
from jax.experimental import pallas as pl
from jax.experimental.pallas import tpu as pltpu
from jax.sharding import PartitionSpec as P

MESH = pl.DeviceIdType.MESH
BF16, F32, I32 = jnp.bfloat16, jnp.float32, jnp.int32
HEAD = 4
COLS = 256
ROOMS = (16, 24, 32, 40, 48, 64)


def greet(n, me, barrier):
    def signal(k, carry):
        pl.semaphore_signal(barrier, inc=1, device_id={"ep": lax.rem(me + k, n)}, device_id_type=MESH)
        return carry
    lax.fori_loop(1, n, signal, 0)


def ffn_kernel(n, fill, need, x, w_gate, w_up, w_down, head_in, own, other, need_all,
               x_buf, gate_buf, up_buf, down_buf, hidden, mask, rows, head,
               load_sem, own_sem, pair_send, pair_recv, head_send, head_recv, need_send, need_recv):
    me = lax.axis_index("ep")
    core = lax.rem(me, 2)
    sources, experts, cap, width = x.shape
    ffn = w_gate.shape[2]
    half = width // 2
    barrier = pltpu.get_barrier_semaphore()
    greet(n, me, barrier)

    def loads(e, slot):
        return (
            pltpu.make_async_copy(x.at[:, e], x_buf.at[slot], load_sem.at[0, slot]),
            pltpu.make_async_copy(w_gate.at[e], gate_buf.at[slot], load_sem.at[1, slot]),
            pltpu.make_async_copy(w_up.at[e], up_buf.at[slot], load_sem.at[2, slot]),
            pltpu.make_async_copy(w_down.at[e], down_buf.at[slot], load_sem.at[3, slot]),
        )

    def own_copy(e):
        return pltpu.make_async_copy(rows.at[e, :, core], own.at[:, e], own_sem.at[e])

    def pair_copy(e):
        return pltpu.make_async_remote_copy(
            src_ref=rows.at[e, :, 1 - core], dst_ref=other.at[:, e], send_sem=pair_send.at[e], recv_sem=pair_recv.at[e],
            device_id={"ep": me + 1 - 2 * core}, device_id_type=MESH)

    for copy in loads(0, 0):
        copy.start()

    def expert(e, carry):
        slot = lax.rem(e, 2)

        @pl.when(e + 1 < experts)
        def _():
            for copy in loads(e + 1, 1 - slot):
                copy.start()

        for s in range(sources):
            live = lax.broadcasted_iota(I32, (cap, 128), 0) < fill[s, e]
            mask[pl.ds(s * cap, cap), :] = jnp.where(live, 1.0, 0.0)
        here = loads(e, slot)
        for copy in here[:3]:
            copy.wait()

        def up(k, carry):
            cols = pl.ds(pl.multiple_of(k * COLS, COLS), COLS)
            act = x_buf[slot].reshape(sources * cap, width)
            a = jnp.dot(act, gate_buf[slot, :, cols], preferred_element_type=F32)
            b = jnp.dot(act, up_buf[slot, :, cols], preferred_element_type=F32)
            hidden[:, cols] = (a * jax.nn.sigmoid(a) * b).astype(BF16)
            return carry
        lax.fori_loop(0, ffn // COLS, up, 0)
        here[3].wait()

        def down(k, carry):
            live = mask[...] > 0.5
            live = jnp.concatenate([live.astype(F32)] * (COLS // 128), axis=1) > 0.5
            tops = []
            for part in range(2):
                cols = pl.ds(pl.multiple_of(part * half + k * COLS, COLS), COLS)
                y = jnp.dot(hidden[...], down_buf[slot, :, cols], preferred_element_type=F32)
                y = jnp.where(live, y, 0.0)
                rows[e, :, :, :, cols] = y.astype(BF16).reshape(sources // 2, 2, cap, COLS)
                tops.append(y.reshape(sources, cap, COLS)[:, :8])
            first = lax.broadcasted_iota(I32, (sources, 8, COLS), 1) < HEAD
            shifted = pltpu.roll(tops[1], HEAD, 1)
            cols = pl.ds(pl.multiple_of(k * COLS, COLS), COLS)
            head[e, :, :, cols] = jnp.where(first, tops[0], shifted).astype(BF16)
            return carry
        lax.fori_loop(0, half // COLS, down, 0)

        @pl.when(e == 0)
        def _():
            pl.semaphore_wait(barrier, n - 1)

            def tell(k, carry):
                to = lax.rem(me + k, n)
                pltpu.make_async_remote_copy(
                    src_ref=need, dst_ref=need_all.at[me], send_sem=need_send, recv_sem=need_recv,
                    device_id={"ep": to}, device_id_type=MESH).start()
                return carry
            lax.fori_loop(1, n, tell, 0)
            pltpu.make_async_copy(need, need_all.at[me], need_recv).start()

        own_copy(e).start()
        pair_copy(e).start()

        def push(k, carry):
            to = lax.rem(me + k, n)
            pltpu.make_async_remote_copy(
                src_ref=head.at[e, to], dst_ref=head_in.at[me * experts + e], send_sem=head_send.at[e],
                recv_sem=head_recv, device_id={"ep": to}, device_id_type=MESH).start()
            return carry
        lax.fori_loop(1, n, push, 0)
        pltpu.make_async_copy(head.at[e, me], head_in.at[me * experts + e], head_recv).start()
        return carry
    lax.fori_loop(0, experts, expert, 0)

    for e in range(experts):
        own_copy(e).wait()
        pair_copy(e).wait()
        sent = head.at[e, pl.ds(0, n - 1)]
        pltpu.make_async_copy(sent, sent, head_send.at[e]).wait()
    pltpu.make_async_copy(head_in, head_in, head_recv).wait()
    pltpu.make_async_copy(need_all, need_all, need_recv).wait()
    sent = need_all.at[pl.ds(0, n - 1)]
    pltpu.make_async_copy(sent, sent, need_send).wait()


def split3(w):
    hi = jnp.minimum(w, 3.3895313892515355e38).astype(BF16)
    rest = w - hi.astype(F32)
    mid = rest.astype(BF16)
    low = (rest - mid.astype(F32)).astype(BF16)
    return hi, mid, low


def tail_kernel(n, room, place, head_key, tail_key, weight, head_in, own, other, out,
                src, pack, got, head_buf, head_mix, tail_mix, total,
                load_sem, head_sem, send_sem, recv_sem):
    me = lax.axis_index("ep")
    core = lax.rem(me, 2)
    chips = n // 2
    chip = me // 2
    tokens, width = out.shape
    half = width // 2
    per = own.shape[1] * own.shape[2]
    barrier = pltpu.get_barrier_semaphore()

    def signal(k, carry):
        to = 2 * lax.rem(chip + k, chips) + core
        pl.semaphore_signal(barrier, inc=1, device_id={"ep": to}, device_id_type=MESH)
        return carry
    lax.fori_loop(1, chips, signal, 0)

    load_own = pltpu.make_async_copy(own, src.at[:, 0], load_sem.at[0])
    load_other = pltpu.make_async_copy(other, src.at[:, 1], load_sem.at[1])
    load_head = pltpu.make_async_copy(head_in, head_buf, head_sem)
    load_own.start()
    load_other.start()
    load_head.start()
    load_own.wait()
    load_other.wait()

    def chunk(j):
        spot = place[j]
        pick = lax.broadcasted_iota(I32, (room, 2 * per), 0) == spot
        pick = jnp.where(pick, 1.0, 0.0).astype(BF16)
        return jnp.dot(pick, src[j].reshape(2 * per, width), preferred_element_type=F32).astype(BF16)

    def send(k):
        j = lax.rem(chip + k, chips)
        return pltpu.make_async_remote_copy(
            src_ref=pack.at[j], dst_ref=got.at[chip], send_sem=send_sem.at[k], recv_sem=recv_sem,
            device_id={"ep": 2 * j + core}, device_id_type=MESH)

    got[chip] = chunk(chip)
    pl.semaphore_wait(barrier, chips - 1)

    def push(k, carry):
        j = lax.rem(chip + k, chips)
        pack[j] = chunk(j)
        send(k).start()
        return carry
    lax.fori_loop(1, chips, push, 0)

    def mix(key_ref, key_add, lanes, mix_ref, base):
        def tile(i, carry):
            lane = lax.broadcasted_iota(I32, (tokens, 128), 1) + i * 128
            w = jnp.zeros((tokens, 128), F32)
            for c in range(key_ref.shape[1]):
                key = key_ref[:, c:c + 1]
                w = w + jnp.where(lane == key + key_add, weight[:, c:c + 1], 0.0)
            cols = pl.ds(pl.multiple_of(i * 128, 128), 128)
            for p, part in enumerate(split3(w)):
                mix_ref[pl.ds(base + p * tokens, tokens), cols] = part
            return carry
        lax.fori_loop(0, lanes // 128, tile, 0)

    head_rows = head_buf.shape[0] * head_buf.shape[1]
    mix(head_key, 0, head_rows, head_mix, 0)
    mix(head_key, HEAD, head_rows, head_mix, 3 * tokens)
    mix(tail_key, 0, chips * room, tail_mix, 0)
    load_head.wait()

    def fold(v, base):
        return v[base:base + tokens] + (v[base + tokens:base + 2 * tokens] + v[base + 2 * tokens:base + 3 * tokens])

    def head_cols(i, carry):
        cols = pl.ds(pl.multiple_of(i * COLS, COLS), COLS)
        v = jnp.dot(head_mix[...], head_buf[:, :, cols].reshape(head_rows, COLS), preferred_element_type=F32)
        total[:, cols] = fold(v, 0)
        total[:, pl.ds(pl.multiple_of(half + i * COLS, COLS), COLS)] = fold(v, 3 * tokens)
        return carry
    lax.fori_loop(0, half // COLS, head_cols, 0)

    taken = got.at[pl.ds(0, chips - 1)]
    pltpu.make_async_copy(taken, taken, recv_sem).wait()

    def tail_cols(i, carry):
        cols = pl.ds(pl.multiple_of(i * COLS, COLS), COLS)
        v = jnp.dot(tail_mix[...], got[:, :, cols].reshape(chips * room, COLS), preferred_element_type=F32)
        out[:, cols] = (total[:, cols] + fold(v, 0)).astype(BF16)
        return carry
    lax.fori_loop(0, width // COLS, tail_cols, 0)

    def sent(k, carry):
        send(k).wait_send()
        return carry
    lax.fori_loop(1, chips, sent, 0)


def solution(mesh):
    n = mesh.shape["ep"]
    chips = n // 2

    def step(dispatched, w_gate, w_up, w_down, fill_count, slot_index, expert_id, gate_weight):
        sources, experts, cap, width = dispatched.shape
        ffn = w_gate.shape[2]
        tokens, top = slot_index.shape
        total_experts = n * experts
        me = lax.axis_index("ep")
        core = lax.rem(me, 2)
        live = slot_index >= 0
        expert = jnp.arange(total_experts, dtype=I32)
        hit = (expert_id[:, :, None] == expert) & live[:, :, None]
        count = jnp.sum(hit.astype(I32), axis=(0, 1))
        beyond = jnp.maximum(count - HEAD, 0)
        per_chip = beyond.reshape(chips, 2 * experts)
        before = jnp.sum(jnp.where((expert[:, None] // (2 * experts) == expert[None, :] // (2 * experts))
                                   & (expert[:, None] < expert[None, :]), beyond[:, None], 0), axis=0)
        most_here = jnp.max(jnp.sum(per_chip, axis=1)).astype(F32)
        need = jnp.concatenate([
            jnp.broadcast_to(most_here, (1, 128)),
            jnp.pad(fill_count.astype(F32).reshape(1, -1), ((0, 0), (0, 128 - sources * experts))),
            jnp.zeros((6, 128), F32)])
        offset = jnp.sum(jnp.where(hit, before[None, None, :], 0), axis=2)
        home = expert_id // (2 * experts)
        head_key = jnp.where(live & (slot_index < HEAD), expert_id * 8 + slot_index, -64)

        any_spec = pl.BlockSpec(memory_space=pl.ANY)
        vmem_spec = pl.BlockSpec(memory_space=pltpu.VMEM)
        smem_spec = pl.BlockSpec(memory_space=pltpu.SMEM)
        shape = jax.ShapeDtypeStruct
        head_in, own, other, need_all = pl.pallas_call(
            functools.partial(ffn_kernel, n),
            name="ffn",
            out_shape=(
                shape((total_experts, 8, width // 2), BF16),
                shape((chips, experts, cap, width), BF16),
                shape((chips, experts, cap, width), BF16),
                shape((n, 8, 128), F32),
            ),
            in_specs=[smem_spec, any_spec] + [any_spec] * 4,
            out_specs=(any_spec,) * 4,
            scratch_shapes=[
                pltpu.VMEM((2, sources, cap, width), BF16),
                pltpu.VMEM((2, width, ffn), BF16),
                pltpu.VMEM((2, width, ffn), BF16),
                pltpu.VMEM((2, ffn, width), BF16),
                pltpu.VMEM((sources * cap, ffn), BF16),
                pltpu.VMEM((sources * cap, 128), F32),
                pltpu.VMEM((experts, sources // 2, 2, cap, width), BF16),
                pltpu.VMEM((experts, sources, 8, width // 2), BF16),
                pltpu.SemaphoreType.DMA((4, 2)),
                pltpu.SemaphoreType.DMA((experts,)),
                pltpu.SemaphoreType.DMA((experts,)),
                pltpu.SemaphoreType.DMA((experts,)),
                pltpu.SemaphoreType.DMA((experts,)),
                pltpu.SemaphoreType.DMA,
                pltpu.SemaphoreType.DMA,
                pltpu.SemaphoreType.DMA,
            ],
            compiler_params=pltpu.CompilerParams(collective_id=0, has_side_effects=True, vmem_limit_bytes=64 * 1024 * 1024 - 65536),
        )(fill_count, need, dispatched, w_gate, w_up, w_down)
        most = jnp.max(need_all[:, 0, 0]).astype(I32)

        def for_core(f):
            f = f.reshape(chips, 2, experts)
            return jnp.where(core == 0, f[:, 0], f[:, 1])
        mine = for_core(fill_count)
        theirs = lax.dynamic_index_in_dim(need_all, me + 1 - 2 * core, 0, keepdims=False)[1, :sources * experts]
        theirs = for_core(theirs.astype(I32).reshape(sources, experts))
        fills = jnp.stack([mine, theirs], axis=1)
        extra = jnp.maximum(fills - HEAD, 0)
        start = jnp.cumsum(extra, axis=2) - extra
        lead = jnp.sum(extra, axis=2)
        start = start + jnp.stack([jnp.where(core == 1, lead[:, 1], 0), jnp.where(core == 0, lead[:, 0], 0)], axis=1)[:, :, None]
        slot = jnp.arange(cap, dtype=I32)
        place = jnp.where((slot >= HEAD) & (slot < fills[..., None]), start[..., None] + slot - HEAD, -1)
        place = place.reshape(chips, 1, 2 * experts * cap)

        def tail(room, index):
            tail_key = jnp.where(live & (slot_index >= HEAD), home * room + offset + slot_index - HEAD, -1)
            return pl.pallas_call(
                functools.partial(tail_kernel, n, room),
                name="tail%d" % room,
                out_shape=shape((tokens, width), BF16),
                in_specs=[vmem_spec] * 4 + [any_spec] * 3,
                out_specs=vmem_spec,
                scratch_shapes=[
                    pltpu.VMEM((chips, 2, experts, cap, width), BF16),
                    pltpu.VMEM((chips, room, width), BF16),
                    pltpu.VMEM((chips, room, width), BF16),
                    pltpu.VMEM((total_experts, 8, width // 2), BF16),
                    pltpu.VMEM((6 * tokens, total_experts * 8), BF16),
                    pltpu.VMEM((3 * tokens, chips * room), BF16),
                    pltpu.VMEM((tokens, width), F32),
                    pltpu.SemaphoreType.DMA((2,)),
                    pltpu.SemaphoreType.DMA,
                    pltpu.SemaphoreType.DMA((chips,)),
                    pltpu.SemaphoreType.DMA,
                ],
                compiler_params=pltpu.CompilerParams(collective_id=1 + index, has_side_effects=True, vmem_limit_bytes=64 * 1024 * 1024 - 65536),
            )(place, head_key, tail_key, gate_weight, head_in, own, other)

        rooms = [r for r in ROOMS if r < 2 * experts * (cap - HEAD)] + [2 * experts * (cap - HEAD)]
        branch = sum([(most > r).astype(I32) for r in rooms[:-1]])
        return lax.switch(branch, [functools.partial(tail, r, i) for i, r in enumerate(rooms)])

    token_spec = P(("dp", "ep"))
    in_specs = (P("dp", "ep"), P("ep"), P("ep"), P("ep"), P("dp", "ep"), token_spec, token_spec, token_spec)
    return jax.shard_map(step, mesh=mesh, in_specs=in_specs, out_specs=token_spec, check_vma=False)
```

```python
import functools
import math

import jax
import jax.numpy as jnp
from jax import lax
from jax.experimental import pallas as pl
from jax.experimental.pallas import tpu as pltpu
from jax.sharding import PartitionSpec as P

MESH = pl.DeviceIdType.MESH
BF16, F32, I32 = jnp.bfloat16, jnp.float32, jnp.int32
HEAD = 4
HEADED = 2
COLS = 256
ROOMS = (24, 32, 40, 48, 56, 64, 80)
GRANT = 64 * 1024 * 1024 - 65536
ORDER = ((2, 2), (1, 2), (3, 2), (2, 1), (2, 3), (1, 1), (3, 3), (1, 3), (3, 1), (2, 0), (0, 2), (1, 0), (3, 0), (0, 1), (0, 3))
STEP_X = sum(x << (2 * i) for i, (x, y) in enumerate(ORDER))
STEP_Y = sum(y << (2 * i) for i, (x, y) in enumerate(ORDER))


def step_to(chip, side, i):
    dx = lax.shift_right_logical(jnp.int32(STEP_X), 2 * i) & 3
    dy = lax.shift_right_logical(jnp.int32(STEP_Y), 2 * i) & 3
    return lax.rem(chip // side + dy, side) * side + lax.rem(lax.rem(chip, side) + dx, side)


def iota(shape, dim):
    return lax.broadcasted_iota(I32, shape, dim)


def one(cond):
    return jnp.where(cond, 1.0, 0.0)


def needs(expert_t, slot_t, total, experts):
    tokens = expert_t.shape[1]
    hit = jnp.zeros((total, tokens), F32)
    for c in range(expert_t.shape[0]):
        hit = hit + one((iota((total, tokens), 0) == expert_t[c:c + 1]) & (slot_t[c:c + 1] >= 0))
    count = jnp.sum(hit, axis=1, keepdims=True)
    headed = lax.rem(iota((total, 1), 0), experts) < HEADED
    beyond = jnp.maximum(count - jnp.where(headed, float(HEAD), 0.0), 0.0)
    g, p = iota((total, total), 0), iota((total, total), 1)
    lower = one((g // (2 * experts) == p // (2 * experts)) & (p < g)).astype(BF16)
    before = jnp.dot(lower, jnp.broadcast_to(beyond, (total, 128)).astype(BF16), preferred_element_type=F32)
    return beyond, before


def ffn_kernel(n, rooms, fill, fill_v, expert_t, slot_t, x, w_gate, w_up, w_down, head_in, own, other, table, branch,
               x_buf, gate_buf, up_buf, down_buf, hidden, mask, rows, head, note,
               load_sem, own_sem, pair_send, pair_recv, head_send, head_recv, note_send, note_recv):
    me = lax.axis_index("ep")
    core = lax.rem(me, 2)
    chip = me // 2
    chips = n // 2
    side = math.isqrt(chips)
    sources, experts, cap, width = x.shape
    ffn = w_gate.shape[2]
    half = width // 2
    barrier = pltpu.get_barrier_semaphore()

    def loads(e, slot):
        return (
            pltpu.make_async_copy(x.at[:, e], x_buf.at[slot], load_sem.at[0, slot]),
            pltpu.make_async_copy(w_gate.at[e], gate_buf.at[slot], load_sem.at[1, slot]),
            pltpu.make_async_copy(w_up.at[e], up_buf.at[slot], load_sem.at[2, slot]),
            pltpu.make_async_copy(w_down.at[e], down_buf.at[slot], load_sem.at[3, slot]),
        )

    for copy in loads(0, 0):
        copy.start()

    def greet(k, carry):
        pl.semaphore_signal(barrier, inc=1, device_id={"ep": lax.rem(me + k, n)}, device_id_type=MESH)
        return carry
    lax.fori_loop(1, n, greet, 0)

    beyond, before = needs(expert_t[...], slot_t[...], n * experts, experts)
    note[...] = jnp.zeros_like(note)
    note[0:experts, 0:sources] = fill_v[...].astype(F32)
    note[experts:experts + 1, :] = jnp.max(before + beyond, axis=0, keepdims=True)

    def own_copy(e):
        return pltpu.make_async_copy(rows.at[e, :, core], own.at[:, e], own_sem.at[e])

    def pair_copy(e):
        return pltpu.make_async_remote_copy(
            src_ref=rows.at[e, :, 1 - core], dst_ref=other.at[:, e], send_sem=pair_send.at[e], recv_sem=pair_recv.at[e],
            device_id={"ep": me + 1 - 2 * core}, device_id_type=MESH)

    def expert(e, carry):
        slot = lax.rem(e, 2)

        @pl.when(e + 1 < experts)
        def _():
            for copy in loads(e + 1, 1 - slot):
                copy.start()

        for s in range(sources):
            mask[pl.ds(s * cap, cap), :] = one(iota((cap, 128), 0) < fill[e, s])
        here = loads(e, slot)
        for copy in here[:3]:
            copy.wait()

        def up(k, carry):
            cols = pl.ds(pl.multiple_of(k * COLS, COLS), COLS)
            act = x_buf[slot].reshape(sources * cap, width)
            a = jnp.dot(act, gate_buf[slot, :, cols], preferred_element_type=F32)
            b = jnp.dot(act, up_buf[slot, :, cols], preferred_element_type=F32)
            hidden[:, cols] = (a * jax.nn.sigmoid(a) * b).astype(BF16)
            return carry
        lax.fori_loop(0, ffn // COLS, up, 0, unroll=True)
        here[3].wait()

        def down(k, carry):
            live = jnp.concatenate([mask[...]] * (COLS // 128), axis=1) > 0.5
            tops = []
            for part in range(2):
                cols = pl.ds(pl.multiple_of(part * half + k * COLS, COLS), COLS)
                y = jnp.dot(hidden[...], down_buf[slot, :, cols], preferred_element_type=F32)
                y = jnp.where(live, y, 0.0)
                rows[e, :, :, :, cols] = y.astype(BF16).reshape(sources // 2, 2, cap, COLS)
                tops.append(y.reshape(sources, cap, COLS)[:, :8])
            first = iota((sources, 8, COLS), 1) < HEAD
            shifted = pltpu.roll(tops[1], HEAD, 1)
            cols = pl.ds(pl.multiple_of(k * COLS, COLS), COLS)
            head[e, :, :, cols] = jnp.where(first, tops[0], shifted).astype(BF16)
            return carry
        lax.fori_loop(0, half // COLS, down, 0, unroll=True)

        @pl.when(e == 0)
        def _():
            pl.semaphore_wait(barrier, n - 1)

            def tell(k, carry):
                pltpu.make_async_remote_copy(
                    src_ref=note, dst_ref=table.at[me], send_sem=note_send, recv_sem=note_recv,
                    device_id={"ep": lax.rem(me + k, n)}, device_id_type=MESH).start()
                return carry
            lax.fori_loop(1, n, tell, 0)
            table[me] = note[...]

        pair_copy(e).start()
        own_copy(e).start()

        @pl.when(e < HEADED)
        def _():
            def push(to):
                pltpu.make_async_remote_copy(
                    src_ref=head.at[e, to], dst_ref=head_in.at[me * HEADED + e], send_sem=head_send.at[e],
                    recv_sem=head_recv, device_id={"ep": to}, device_id_type=MESH).start()

            def same(i, carry):
                push(2 * step_to(chip, side, i) + core)
                return carry

            def cross(i, carry):
                push(2 * step_to(chip, side, i) + 1 - core)
                return carry
            lax.fori_loop(0, chips - 1, same, 0)
            lax.fori_loop(0, chips - 1, cross, 0)
            push(2 * chip + 1 - core)
            pltpu.make_async_copy(head.at[e, me], head_in.at[me * HEADED + e], head_recv).start()
        return carry
    lax.fori_loop(0, experts, expert, 0)

    got = table.at[pl.ds(0, n - 1)]
    pltpu.make_async_copy(got, got, note_recv).wait()
    pltpu.make_async_copy(got, got, note_send).wait()
    most = jnp.max(jnp.max(table[...], axis=0)[experts:experts + 1, :])
    index = jnp.int32(0)
    for room in rooms[:-1]:
        index = index + (most > float(room)).astype(I32)
    branch[0, 0] = index
    for e in range(experts):
        own_copy(e).wait()
        pair_copy(e).wait()
        if e < HEADED:
            sent = head.at[e, pl.ds(0, n - 1)]
            pltpu.make_async_copy(sent, sent, head_send.at[e]).wait()
    pltpu.make_async_copy(head_in, head_in, head_recv).wait()


def split3(w):
    hi = jnp.minimum(w, 3.3895313892515355e38).astype(BF16)
    rest = w - hi.astype(F32)
    mid = rest.astype(BF16)
    low = (rest - mid.astype(F32)).astype(BF16)
    return hi, mid, low


def tail_kernel(n, room, table, expert_t, slot_t, weight_t, head_in, own, other, out,
                src, pack, got, head_buf, head_mix, tail_mix, total, place, keys,
                load_sem, head_sem, send_sem, recv_sem):
    me = lax.axis_index("ep")
    core = lax.rem(me, 2)
    chip = me // 2
    chips = n // 2
    side = math.isqrt(chips)
    _, experts, cap, width = own.shape
    tokens = out.shape[0]
    half = width // 2
    per = experts * cap
    lanes = 2 * per
    barrier = pltpu.get_barrier_semaphore()

    def greet(i, carry):
        pl.semaphore_signal(barrier, inc=1, device_id={"ep": 2 * step_to(chip, side, i) + core}, device_id_type=MESH)
        return carry
    lax.fori_loop(0, chips - 1, greet, 0)

    def load(i, j):
        return (pltpu.make_async_copy(own.at[j], src.at[i, 0], load_sem.at[i, 0]),
                pltpu.make_async_copy(other.at[j], src.at[i, 1], load_sem.at[i, 1]))

    def load_to(i, carry):
        for copy in load(i, step_to(chip, side, i)):
            copy.start()
        return carry
    lax.fori_loop(0, chips - 1, load_to, 0)
    for copy in load(chips - 1, chip):
        copy.start()
    load_head = pltpu.make_async_copy(head_in, head_buf, head_sem)
    load_head.start()

    fills = jnp.concatenate([table[me, 0:experts], table[me + 1 - 2 * core, 0:experts], jnp.zeros((128 - 2 * experts, 128), F32)])
    fills = fills.T
    k, lane = iota((128, lanes), 0), iota((128, lanes), 1)
    early = lax.rem(iota((128, 128), 1), experts) < HEADED
    extra = jnp.maximum(fills - jnp.where(early, float(HEAD), 0.0), 0.0)
    rank_k = lax.rem(k + experts * core, 2 * experts)
    rank_l = lax.rem(lane // cap + experts * core, 2 * experts)
    spread = one(k == lane // cap).astype(BF16)
    earlier = one((rank_k < rank_l) & (k < 2 * experts)).astype(BF16)
    filled = jnp.dot(fills.astype(BF16), spread, preferred_element_type=F32)
    start = jnp.dot(extra.astype(BF16), earlier, preferred_element_type=F32)
    lane = iota((128, lanes), 1)
    slot = lax.rem(lane, cap)
    skip = jnp.where(lax.rem(lane // cap, experts) < HEADED, HEAD, 0)
    spot = jnp.where((slot >= skip) & (slot.astype(F32) < filled), start.astype(I32) + slot - skip, -1)
    place[...] = spot[0:n]

    def chunk(i, j):
        for copy in load(i, j):
            copy.wait()
        pick = one(iota((room, lanes), 0) == place[pl.ds(2 * j + core, 1), :]).astype(BF16)
        return jnp.dot(pick, src[i].reshape(lanes, width), preferred_element_type=F32).astype(BF16)

    def send(i, j):
        return pltpu.make_async_remote_copy(
            src_ref=pack.at[i], dst_ref=got.at[i], send_sem=send_sem.at[i], recv_sem=recv_sem,
            device_id={"ep": 2 * j + core}, device_id_type=MESH)

    pl.semaphore_wait(barrier, chips - 1)

    def push(i, carry):
        j = step_to(chip, side, i)
        pack[i] = chunk(i, j)
        send(i, j).start()
        return carry
    lax.fori_loop(0, chips - 1, push, 0)
    got[chips - 1] = chunk(chips - 1, chip)

    total_experts = n * experts
    expert, slot = expert_t[...], slot_t[...]
    top = expert.shape[0]
    beyond, before = needs(expert, slot, total_experts, experts)
    lead = []
    for c in range(top):
        hit = iota((total_experts, tokens), 0) == expert[c:c + 1]
        lead.append(jnp.sum(jnp.where(hit, before, 0.0), axis=0, keepdims=True))
    lead = jnp.concatenate(lead, axis=0).astype(I32)
    local = lax.rem(expert, experts)
    early = local < HEADED
    in_head = early & (slot >= 0) & (slot < HEAD)
    head_key = jnp.where(in_head, ((expert // experts) * HEADED + local) * 8 + slot, -64)
    home = expert // (2 * experts)
    base = jnp.full(expert.shape, (chips - 1) * room, I32)
    for i, (dx, dy) in enumerate(ORDER):
        came = lax.rem(chip // side + side - dy, side) * side + lax.rem(lax.rem(chip, side) + side - dx, side)
        base = jnp.where(home == came, i * room, base)
    skip = jnp.where(early, HEAD, 0)
    tail_key = jnp.where(slot >= skip, base + lead + slot - skip, -64)
    stack = jnp.concatenate([head_key.astype(F32), tail_key.astype(F32), weight_t[...], jnp.zeros((128 - 3 * top, tokens), F32)])
    keys[...] = stack.T

    def mix(first, add, count, mix_ref, base):
        def tile(i, carry):
            lane = (iota((tokens, 128), 1) + (i * 128 - add)).astype(F32)
            w = jnp.zeros((tokens, 128), F32)
            for c in range(top):
                w = w + jnp.where(lane == keys[:, first + c:first + c + 1], keys[:, 2 * top + c:2 * top + c + 1], 0.0)
            cols = pl.ds(pl.multiple_of(i * 128, 128), 128)
            for p, part in enumerate(split3(w)):
                mix_ref[pl.ds(base + p * tokens, tokens), cols] = part
            return carry
        lax.fori_loop(0, count // 128, tile, 0)

    head_rows = head_buf.shape[0] * head_buf.shape[1]
    mix(0, 0, head_rows, head_mix, 0)
    mix(0, HEAD, head_rows, head_mix, 3 * tokens)
    mix(top, 0, chips * room, tail_mix, 0)
    load_head.wait()

    def fold(v, base):
        return v[base:base + tokens] + (v[base + tokens:base + 2 * tokens] + v[base + 2 * tokens:base + 3 * tokens])

    def head_cols(i, carry):
        cols = pl.ds(pl.multiple_of(i * COLS, COLS), COLS)
        v = jnp.dot(head_mix[...], head_buf[:, :, cols].reshape(head_rows, COLS), preferred_element_type=F32)
        total[:, cols] = fold(v, 0)
        total[:, pl.ds(pl.multiple_of(half + i * COLS, COLS), COLS)] = fold(v, 3 * tokens)
        return carry
    lax.fori_loop(0, half // COLS, head_cols, 0)

    taken = got.at[pl.ds(0, chips - 1)]
    pltpu.make_async_copy(taken, taken, recv_sem).wait()

    def tail_cols(i, carry):
        cols = pl.ds(pl.multiple_of(i * COLS, COLS), COLS)
        v = jnp.dot(tail_mix[...], got[:, :, cols].reshape(chips * room, COLS), preferred_element_type=F32)
        out[:, cols] = (total[:, cols] + fold(v, 0)).astype(BF16)
        return carry
    lax.fori_loop(0, width // COLS, tail_cols, 0, unroll=True)

    def sent(i, carry):
        send(i, step_to(chip, side, i)).wait_send()
        return carry
    lax.fori_loop(0, chips - 1, sent, 0)


def solution(mesh):
    n = mesh.shape["ep"]
    chips = n // 2

    def step(dispatched, w_gate, w_up, w_down, fill_count, slot_index, expert_id, gate_weight):
        sources, experts, cap, width = dispatched.shape
        ffn = w_gate.shape[2]
        tokens, top = slot_index.shape
        most = 2 * (HEADED * (cap - HEAD) + (experts - HEADED) * cap)
        rooms = [r for r in ROOMS if r < most] + [most]
        any_spec = pl.BlockSpec(memory_space=pl.ANY)
        vmem_spec = pl.BlockSpec(memory_space=pltpu.VMEM)
        smem_spec = pl.BlockSpec(memory_space=pltpu.SMEM)
        shape = jax.ShapeDtypeStruct
        dma = pltpu.SemaphoreType.DMA
        fill_t, expert_t, slot_t, weight_t = fill_count.T, expert_id.T, slot_index.T, gate_weight.T
        head_in, own, other, table, branch = pl.pallas_call(
            functools.partial(ffn_kernel, n, rooms),
            name="ffn",
            out_shape=(
                shape((n * HEADED, 8, width // 2), BF16),
                shape((chips, experts, cap, width), BF16),
                shape((chips, experts, cap, width), BF16),
                shape((n, 8, 128), F32),
                shape((1, 1), I32),
            ),
            in_specs=[smem_spec] + [vmem_spec] * 3 + [any_spec] * 4,
            out_specs=(any_spec,) * 3 + (vmem_spec, smem_spec),
            scratch_shapes=[
                pltpu.VMEM((2, sources, cap, width), BF16),
                pltpu.VMEM((2, width, ffn), BF16),
                pltpu.VMEM((2, width, ffn), BF16),
                pltpu.VMEM((2, ffn, width), BF16),
                pltpu.VMEM((sources * cap, ffn), BF16),
                pltpu.VMEM((sources * cap, 128), F32),
                pltpu.VMEM((experts, sources // 2, 2, cap, width), BF16),
                pltpu.VMEM((experts, sources, 8, width // 2), BF16),
                pltpu.VMEM((8, 128), F32),
                dma((4, 2)), dma((experts,)), dma((experts,)), dma((experts,)), dma((HEADED,)), dma, dma, dma,
            ],
            compiler_params=pltpu.CompilerParams(collective_id=0, has_side_effects=True, vmem_limit_bytes=GRANT),
        )(fill_t, fill_t, expert_t, slot_t, dispatched, w_gate, w_up, w_down)

        def tail(room, index):
            return pl.pallas_call(
                functools.partial(tail_kernel, n, room),
                name="tail%d" % room,
                out_shape=shape((tokens, width), BF16),
                in_specs=[vmem_spec] * 4 + [any_spec] * 3,
                out_specs=vmem_spec,
                scratch_shapes=[
                    pltpu.VMEM((chips, 2, experts, cap, width), BF16),
                    pltpu.VMEM((chips, room, width), BF16),
                    pltpu.VMEM((chips, room, width), BF16),
                    pltpu.VMEM((n * HEADED, 8, width // 2), BF16),
                    pltpu.VMEM((6 * tokens, n * HEADED * 8), BF16),
                    pltpu.VMEM((3 * tokens, chips * room), BF16),
                    pltpu.VMEM((tokens, width), F32),
                    pltpu.VMEM((n, 2 * experts * cap), I32),
                    pltpu.VMEM((tokens, 128), F32),
                    dma((chips, 2)), dma, dma((chips,)), dma,
                ],
                compiler_params=pltpu.CompilerParams(collective_id=1 + index, has_side_effects=True, vmem_limit_bytes=GRANT),
            )(table, expert_t, slot_t, weight_t, head_in, own, other)

        return lax.switch(branch[0, 0], [functools.partial(tail, r, i) for i, r in enumerate(rooms)])

    token_spec = P(("dp", "ep"))
    in_specs = (P("dp", "ep"), P("ep"), P("ep"), P("ep"), P("dp", "ep"), token_spec, token_spec, token_spec)
    return jax.shard_map(step, mesh=mesh, in_specs=in_specs, out_specs=token_spec, check_vma=False)
```

```python
import functools
import math

import jax
import jax.numpy as jnp
from jax import lax
from jax.experimental import pallas as pl
from jax.experimental.pallas import tpu as pltpu
from jax.sharding import PartitionSpec as P

MESH = pl.DeviceIdType.MESH
BF16, F32, I32 = jnp.bfloat16, jnp.float32, jnp.int32
HEAD = 4
HEADED = 3
COLS = 256
ROOMS = (24, 32, 40, 48, 56, 64, 80)
GRANT = 64 * 1024 * 1024 - 65536
ORDER = ((2, 2), (2, 1), (2, 3), (1, 2), (3, 2), (2, 0), (0, 2), (1, 1), (3, 3), (1, 3), (3, 1), (1, 0), (3, 0), (0, 1), (0, 3))
STEP_X = sum(x << (2 * i) for i, (x, y) in enumerate(ORDER))
STEP_Y = sum(y << (2 * i) for i, (x, y) in enumerate(ORDER))


def step_to(chip, side, i):
    dx = lax.shift_right_logical(jnp.int32(STEP_X), 2 * i) & 3
    dy = lax.shift_right_logical(jnp.int32(STEP_Y), 2 * i) & 3
    return lax.rem(chip // side + dy, side) * side + lax.rem(lax.rem(chip, side) + dx, side)


def iota(shape, dim):
    return lax.broadcasted_iota(I32, shape, dim)


def one(cond):
    return jnp.where(cond, 1.0, 0.0)


def needs(expert_t, slot_t, total, experts):
    tokens = expert_t.shape[1]
    hit = jnp.zeros((total, tokens), F32)
    for c in range(expert_t.shape[0]):
        hit = hit + one((iota((total, tokens), 0) == expert_t[c:c + 1]) & (slot_t[c:c + 1] >= 0))
    count = jnp.sum(hit, axis=1, keepdims=True)
    headed = lax.rem(iota((total, 1), 0), experts) < HEADED
    beyond = jnp.maximum(count - jnp.where(headed, float(HEAD), 0.0), 0.0)
    g, p = iota((total, total), 0), iota((total, total), 1)
    lower = one((g // (2 * experts) == p // (2 * experts)) & (p < g)).astype(BF16)
    before = jnp.dot(lower, jnp.broadcast_to(beyond, (total, 128)).astype(BF16), preferred_element_type=F32)
    return beyond, before


def ffn_kernel(n, rooms, fill, fill_v, expert_t, slot_t, x, w_gate, w_up, w_down, head_in, own, other, table, branch,
               x_buf, gate_buf, up_buf, down_buf, hidden, mask, rows, head, note,
               load_sem, own_sem, pair_send, pair_recv, head_send, head_recv, note_send, note_recv):
    me = lax.axis_index("ep")
    core = lax.rem(me, 2)
    chip = me // 2
    chips = n // 2
    side = math.isqrt(chips)
    sources, experts, cap, width = x.shape
    ffn = w_gate.shape[2]
    half = width // 2
    barrier = pltpu.get_barrier_semaphore()

    def loads(e, slot):
        return (
            pltpu.make_async_copy(x.at[:, e], x_buf.at[slot], load_sem.at[0, slot]),
            pltpu.make_async_copy(w_gate.at[e], gate_buf.at[slot], load_sem.at[1, slot]),
            pltpu.make_async_copy(w_up.at[e], up_buf.at[slot], load_sem.at[2, slot]),
            pltpu.make_async_copy(w_down.at[e], down_buf.at[slot], load_sem.at[3, slot]),
        )

    for copy in loads(0, 0):
        copy.start()

    def greet(k, carry):
        pl.semaphore_signal(barrier, inc=1, device_id={"ep": lax.rem(me + k, n)}, device_id_type=MESH)
        return carry
    lax.fori_loop(1, n, greet, 0)

    beyond, before = needs(expert_t[...], slot_t[...], n * experts, experts)
    note[...] = jnp.zeros_like(note)
    note[0:experts, 0:sources] = fill_v[...].astype(F32)
    note[experts:experts + 1, :] = jnp.max(before + beyond, axis=0, keepdims=True)

    def own_copy(e):
        return pltpu.make_async_copy(rows.at[e, :, core], own.at[:, e], own_sem.at[e])

    def pair_copy(e):
        return pltpu.make_async_remote_copy(
            src_ref=rows.at[e, :, 1 - core], dst_ref=other.at[:, e], send_sem=pair_send.at[e], recv_sem=pair_recv.at[e],
            device_id={"ep": me + 1 - 2 * core}, device_id_type=MESH)

    def expert(e, carry):
        slot = lax.rem(e, 2)

        @pl.when(e + 1 < experts)
        def _():
            for copy in loads(e + 1, 1 - slot):
                copy.start()

        for s in range(sources):
            mask[pl.ds(s * cap, cap), :] = one(iota((cap, 128), 0) < fill[e, s])
        here = loads(e, slot)
        for copy in here[:3]:
            copy.wait()

        def up(k, carry):
            cols = pl.ds(pl.multiple_of(k * COLS, COLS), COLS)
            act = x_buf[slot].reshape(sources * cap, width)
            a = jnp.dot(act, gate_buf[slot, :, cols], preferred_element_type=F32)
            b = jnp.dot(act, up_buf[slot, :, cols], preferred_element_type=F32)
            hidden[:, cols] = (a * jax.nn.sigmoid(a) * b).astype(BF16)
            return carry
        lax.fori_loop(0, ffn // COLS, up, 0, unroll=True)
        here[3].wait()

        def down(k, carry):
            live = jnp.concatenate([mask[...]] * (COLS // 128), axis=1) > 0.5
            tops = []
            for part in range(2):
                cols = pl.ds(pl.multiple_of(part * half + k * COLS, COLS), COLS)
                y = jnp.dot(hidden[...], down_buf[slot, :, cols], preferred_element_type=F32)
                y = jnp.where(live, y, 0.0)
                rows[e, :, :, :, cols] = y.astype(BF16).reshape(sources // 2, 2, cap, COLS)
                tops.append(y.reshape(sources, cap, COLS)[:, :8])
            first = iota((sources, 8, COLS), 1) < HEAD
            shifted = pltpu.roll(tops[1], HEAD, 1)
            cols = pl.ds(pl.multiple_of(k * COLS, COLS), COLS)
            head[e, :, :, cols] = jnp.where(first, tops[0], shifted).astype(BF16)
            return carry
        lax.fori_loop(0, half // COLS, down, 0, unroll=True)

        @pl.when(e == 0)
        def _():
            pl.semaphore_wait(barrier, n - 1)

            def tell(k, carry):
                pltpu.make_async_remote_copy(
                    src_ref=note, dst_ref=table.at[me], send_sem=note_send, recv_sem=note_recv,
                    device_id={"ep": lax.rem(me + k, n)}, device_id_type=MESH).start()
                return carry
            lax.fori_loop(1, n, tell, 0)
            table[me] = note[...]

        pair_copy(e).start()
        own_copy(e).start()

        @pl.when(e < HEADED)
        def _():
            def push(to):
                pltpu.make_async_remote_copy(
                    src_ref=head.at[e, to], dst_ref=head_in.at[me * HEADED + e], send_sem=head_send.at[e],
                    recv_sem=head_recv, device_id={"ep": to}, device_id_type=MESH).start()

            def same(i, carry):
                push(2 * step_to(chip, side, i) + core)
                return carry

            def cross(i, carry):
                push(2 * step_to(chip, side, i) + 1 - core)
                return carry
            lax.fori_loop(0, chips - 1, same, 0)
            lax.fori_loop(0, chips - 1, cross, 0)
            push(2 * chip + 1 - core)
            pltpu.make_async_copy(head.at[e, me], head_in.at[me * HEADED + e], head_recv).start()
        return carry
    lax.fori_loop(0, experts, expert, 0)

    got = table.at[pl.ds(0, n - 1)]
    pltpu.make_async_copy(got, got, note_recv).wait()
    pltpu.make_async_copy(got, got, note_send).wait()
    most = jnp.max(jnp.max(table[...], axis=0)[experts:experts + 1, :])
    index = jnp.int32(0)
    for room in rooms[:-1]:
        index = index + (most > float(room)).astype(I32)
    branch[0, 0] = index
    for e in range(experts):
        own_copy(e).wait()
        pair_copy(e).wait()
        if e < HEADED:
            sent = head.at[e, pl.ds(0, n - 1)]
            pltpu.make_async_copy(sent, sent, head_send.at[e]).wait()
    pltpu.make_async_copy(head_in, head_in, head_recv).wait()


def split3(w):
    hi = jnp.minimum(w, 3.3895313892515355e38).astype(BF16)
    rest = w - hi.astype(F32)
    mid = rest.astype(BF16)
    low = (rest - mid.astype(F32)).astype(BF16)
    return hi, mid, low


def tail_kernel(n, room, table, expert_t, slot_t, weight_t, head_in, own, other, out,
                src, pack_a, pack_b, got_a, got_b, head_buf, head_mix, mix_a, mix_b, total, place, keys,
                load_sem, head_sem, send_sem, recv_sem):
    me = lax.axis_index("ep")
    core = lax.rem(me, 2)
    chip = me // 2
    chips = n // 2
    side = math.isqrt(chips)
    _, experts, cap, width = own.shape
    tokens = out.shape[0]
    half = width // 2
    per = experts * cap
    lanes = 2 * per
    barrier = pltpu.get_barrier_semaphore()

    def greet(i, carry):
        pl.semaphore_signal(barrier, inc=1, device_id={"ep": 2 * step_to(chip, side, i) + core}, device_id_type=MESH)
        return carry
    lax.fori_loop(0, chips - 1, greet, 0)

    def load(i, j):
        return (pltpu.make_async_copy(own.at[j], src.at[i, 0], load_sem.at[i, 0]),
                pltpu.make_async_copy(other.at[j], src.at[i, 1], load_sem.at[i, 1]))

    def load_to(i, carry):
        for copy in load(i, step_to(chip, side, i)):
            copy.start()
        return carry
    lax.fori_loop(0, chips - 1, load_to, 0)
    for copy in load(chips - 1, chip):
        copy.start()
    load_head = pltpu.make_async_copy(head_in, head_buf, head_sem)
    load_head.start()

    fills = jnp.concatenate([table[me, 0:experts], table[me + 1 - 2 * core, 0:experts], jnp.zeros((128 - 2 * experts, 128), F32)])
    fills = fills.T
    k, lane = iota((128, lanes), 0), iota((128, lanes), 1)
    early = lax.rem(iota((128, 128), 1), experts) < HEADED
    extra = jnp.maximum(fills - jnp.where(early, float(HEAD), 0.0), 0.0)
    rank_k = lax.rem(k + experts * core, 2 * experts)
    rank_l = lax.rem(lane // cap + experts * core, 2 * experts)
    spread = one(k == lane // cap).astype(BF16)
    earlier = one((rank_k < rank_l) & (k < 2 * experts)).astype(BF16)
    filled = jnp.dot(fills.astype(BF16), spread, preferred_element_type=F32)
    start = jnp.dot(extra.astype(BF16), earlier, preferred_element_type=F32)
    lane = iota((128, lanes), 1)
    slot = lax.rem(lane, cap)
    skip = jnp.where(lax.rem(lane // cap, experts) < HEADED, HEAD, 0)
    spot = jnp.where((slot >= skip) & (slot.astype(F32) < filled), start.astype(I32) + slot - skip, -1)
    place[...] = spot[0:n]

    def chunk(i, j):
        for copy in load(i, j):
            copy.wait()
        pick = one(iota((room, lanes), 0) == place[pl.ds(2 * j + core, 1), :]).astype(BF16)
        return jnp.dot(pick, src[i].reshape(lanes, width), preferred_element_type=F32).astype(BF16)

    def send(p, i, j):
        return pltpu.make_async_remote_copy(
            src_ref=(pack_a, pack_b)[p].at[i], dst_ref=(got_a, got_b)[p].at[i], send_sem=send_sem.at[p],
            recv_sem=recv_sem.at[p], device_id={"ep": 2 * j + core}, device_id_type=MESH)

    cut = got_a.shape[1]

    pl.semaphore_wait(barrier, chips - 1)

    def push(i, carry):
        j = step_to(chip, side, i)
        block = chunk(i, j)
        pack_a[i] = block[:cut]
        pack_b[i] = block[cut:]
        send(0, i, j).start()
        return carry
    lax.fori_loop(0, chips - 1, push, 0)

    def push_rest(i, carry):
        send(1, i, step_to(chip, side, i)).start()
        return carry
    lax.fori_loop(0, chips - 1, push_rest, 0)
    block = chunk(chips - 1, chip)
    got_a[chips - 1] = block[:cut]
    got_b[chips - 1] = block[cut:]

    total_experts = n * experts
    expert, slot = expert_t[...], slot_t[...]
    top = expert.shape[0]
    beyond, before = needs(expert, slot, total_experts, experts)
    lead = []
    for c in range(top):
        hit = iota((total_experts, tokens), 0) == expert[c:c + 1]
        lead.append(jnp.sum(jnp.where(hit, before, 0.0), axis=0, keepdims=True))
    lead = jnp.concatenate(lead, axis=0).astype(I32)
    local = lax.rem(expert, experts)
    early = local < HEADED
    in_head = early & (slot >= 0) & (slot < HEAD)
    head_key = jnp.where(in_head, ((expert // experts) * HEADED + local) * 8 + slot, -64)
    home = expert // (2 * experts)
    order = jnp.full(expert.shape, chips - 1, I32)
    for i, (dx, dy) in enumerate(ORDER):
        came = lax.rem(chip // side + side - dy, side) * side + lax.rem(lax.rem(chip, side) + side - dx, side)
        order = jnp.where(home == came, i, order)
    skip = jnp.where(early, HEAD, 0)
    spot = lead + slot - skip
    rest = room - cut
    key_a = jnp.where((slot >= skip) & (spot < cut), order * cut + spot, -64)
    key_b = jnp.where((slot >= skip) & (spot >= cut), order * rest + spot - cut, -64)
    stack = [key.astype(F32) for key in (head_key, key_a, key_b)]
    stack = jnp.concatenate(stack + [weight_t[...], jnp.zeros((128 - 4 * top, tokens), F32)])
    keys[...] = stack.T

    def mix(first, add, count, mix_ref, base):
        def tile(i, carry):
            lane = (iota((tokens, 128), 1) + (i * 128 - add)).astype(F32)
            w = jnp.zeros((tokens, 128), F32)
            for c in range(top):
                w = w + jnp.where(lane == keys[:, first + c:first + c + 1], keys[:, 3 * top + c:3 * top + c + 1], 0.0)
            cols = pl.ds(pl.multiple_of(i * 128, 128), 128)
            for p, part in enumerate(split3(w)):
                mix_ref[pl.ds(base + p * tokens, tokens), cols] = part
            return carry
        lax.fori_loop(0, count // 128, tile, 0)

    head_rows = head_buf.shape[0] * head_buf.shape[1]
    mix(0, 0, head_rows, head_mix, 0)
    mix(0, HEAD, head_rows, head_mix, 3 * tokens)
    mix(top, 0, chips * cut, mix_a, 0)
    mix(2 * top, 0, chips * rest, mix_b, 0)
    load_head.wait()

    def fold(v, base):
        return v[base:base + tokens] + (v[base + tokens:base + 2 * tokens] + v[base + 2 * tokens:base + 3 * tokens])

    def head_cols(i, carry):
        cols = pl.ds(pl.multiple_of(i * COLS, COLS), COLS)
        v = jnp.dot(head_mix[...], head_buf[:, :, cols].reshape(head_rows, COLS), preferred_element_type=F32)
        total[:, cols] = fold(v, 0)
        total[:, pl.ds(pl.multiple_of(half + i * COLS, COLS), COLS)] = fold(v, 3 * tokens)
        return carry
    lax.fori_loop(0, half // COLS, head_cols, 0)

    def arrived(p):
        taken = (got_a, got_b)[p].at[pl.ds(0, chips - 1)]
        pltpu.make_async_copy(taken, taken, recv_sem.at[p]).wait()

    def part(got, mix_ref, cols):
        rows = got.shape[0] * got.shape[1]
        return fold(jnp.dot(mix_ref[...], got[:, :, cols].reshape(rows, COLS), preferred_element_type=F32), 0)

    arrived(0)

    def first_cols(i, carry):
        cols = pl.ds(pl.multiple_of(i * COLS, COLS), COLS)
        total[:, cols] += part(got_a, mix_a, cols)
        return carry
    lax.fori_loop(0, width // COLS, first_cols, 0)
    arrived(1)

    def last_cols(i, carry):
        cols = pl.ds(pl.multiple_of(i * COLS, COLS), COLS)
        out[:, cols] = (total[:, cols] + part(got_b, mix_b, cols)).astype(BF16)
        return carry
    lax.fori_loop(0, width // COLS, last_cols, 0, unroll=True)

    for p in range(2):
        sent = (pack_a, pack_b)[p]
        pltpu.make_async_copy(sent, sent, send_sem.at[p]).wait()


def solution(mesh):
    n = mesh.shape["ep"]
    chips = n // 2

    def step(dispatched, w_gate, w_up, w_down, fill_count, slot_index, expert_id, gate_weight):
        sources, experts, cap, width = dispatched.shape
        ffn = w_gate.shape[2]
        tokens, top = slot_index.shape
        most = 2 * (HEADED * (cap - HEAD) + (experts - HEADED) * cap)
        rooms = [r for r in ROOMS if r < most] + [most]
        any_spec = pl.BlockSpec(memory_space=pl.ANY)
        vmem_spec = pl.BlockSpec(memory_space=pltpu.VMEM)
        smem_spec = pl.BlockSpec(memory_space=pltpu.SMEM)
        shape = jax.ShapeDtypeStruct
        dma = pltpu.SemaphoreType.DMA
        fill_t, expert_t, slot_t, weight_t = fill_count.T, expert_id.T, slot_index.T, gate_weight.T
        head_in, own, other, table, branch = pl.pallas_call(
            functools.partial(ffn_kernel, n, rooms),
            name="ffn",
            out_shape=(
                shape((n * HEADED, 8, width // 2), BF16),
                shape((chips, experts, cap, width), BF16),
                shape((chips, experts, cap, width), BF16),
                shape((n, 8, 128), F32),
                shape((1, 1), I32),
            ),
            in_specs=[smem_spec] + [vmem_spec] * 3 + [any_spec] * 4,
            out_specs=(any_spec,) * 3 + (vmem_spec, smem_spec),
            scratch_shapes=[
                pltpu.VMEM((2, sources, cap, width), BF16),
                pltpu.VMEM((2, width, ffn), BF16),
                pltpu.VMEM((2, width, ffn), BF16),
                pltpu.VMEM((2, ffn, width), BF16),
                pltpu.VMEM((sources * cap, ffn), BF16),
                pltpu.VMEM((sources * cap, 128), F32),
                pltpu.VMEM((experts, sources // 2, 2, cap, width), BF16),
                pltpu.VMEM((experts, sources, 8, width // 2), BF16),
                pltpu.VMEM((8, 128), F32),
                dma((4, 2)), dma((experts,)), dma((experts,)), dma((experts,)), dma((HEADED,)), dma, dma, dma,
            ],
            compiler_params=pltpu.CompilerParams(collective_id=0, has_side_effects=True, vmem_limit_bytes=GRANT),
        )(fill_t, fill_t, expert_t, slot_t, dispatched, w_gate, w_up, w_down)

        def tail(room, index):
            cut = -(-room // 16) * 8
            return pl.pallas_call(
                functools.partial(tail_kernel, n, room),
                name="tail%d" % room,
                out_shape=shape((tokens, width), BF16),
                in_specs=[vmem_spec] * 4 + [any_spec] * 3,
                out_specs=vmem_spec,
                scratch_shapes=[
                    pltpu.VMEM((chips, 2, experts, cap, width), BF16),
                    pltpu.VMEM((chips - 1, cut, width), BF16),
                    pltpu.VMEM((chips - 1, room - cut, width), BF16),
                    pltpu.VMEM((chips, cut, width), BF16),
                    pltpu.VMEM((chips, room - cut, width), BF16),
                    pltpu.VMEM((n * HEADED, 8, width // 2), BF16),
                    pltpu.VMEM((6 * tokens, n * HEADED * 8), BF16),
                    pltpu.VMEM((3 * tokens, chips * cut), BF16),
                    pltpu.VMEM((3 * tokens, chips * (room - cut)), BF16),
                    pltpu.VMEM((tokens, width), F32),
                    pltpu.VMEM((n, 2 * experts * cap), I32),
                    pltpu.VMEM((tokens, 128), F32),
                    dma((chips, 2)), dma, dma((2,)), dma((2,)),
                ],
                compiler_params=pltpu.CompilerParams(collective_id=1 + index, has_side_effects=True, vmem_limit_bytes=GRANT),
            )(table, expert_t, slot_t, weight_t, head_in, own, other)

        return lax.switch(branch[0, 0], [functools.partial(tail, r, i) for i, r in enumerate(rooms)])

    token_spec = P(("dp", "ep"))
    in_specs = (P("dp", "ep"), P("ep"), P("ep"), P("ep"), P("dp", "ep"), token_spec, token_spec, token_spec)
    return jax.shard_map(step, mesh=mesh, in_specs=in_specs, out_specs=token_spec, check_vma=False)
```

```python
import functools
import math

import jax
import jax.numpy as jnp
from jax import lax
from jax.experimental import pallas as pl
from jax.experimental.pallas import tpu as pltpu
from jax.sharding import PartitionSpec as P

MESH = pl.DeviceIdType.MESH
BF16, F32, I32 = jnp.bfloat16, jnp.float32, jnp.int32
HEAD = 4
HEADED = 3
COLS = 256
ROOM = 48
MORE = (8, 16, 24, 40)
GRANT = 64 * 1024 * 1024 - 65536
ORDER = ((2, 2), (2, 1), (2, 3), (1, 2), (3, 2), (2, 0), (0, 2), (1, 1), (3, 3), (1, 3), (3, 1), (1, 0), (3, 0), (0, 1), (0, 3))
STEP_X = sum(x << (2 * i) for i, (x, y) in enumerate(ORDER))
STEP_Y = sum(y << (2 * i) for i, (x, y) in enumerate(ORDER))


def step_to(chip, side, i):
    dx = lax.shift_right_logical(jnp.int32(STEP_X), 2 * i) & 3
    dy = lax.shift_right_logical(jnp.int32(STEP_Y), 2 * i) & 3
    return ((chip + dy * side) & (side * side - side)) + ((chip + dx) & (side - 1))


def iota(shape, dim):
    return lax.broadcasted_iota(I32, shape, dim)


def one(cond):
    return jnp.where(cond, 1.0, 0.0)


def needs(expert_t, slot_t, total, experts):
    tokens = expert_t.shape[1]
    hit = jnp.zeros((total, tokens), F32)
    for c in range(expert_t.shape[0]):
        hit = hit + one((iota((total, tokens), 0) == expert_t[c:c + 1]) & (slot_t[c:c + 1] >= 0))
    count = jnp.sum(hit, axis=1, keepdims=True)
    headed = lax.rem(iota((total, 1), 0), experts) < HEADED
    beyond = jnp.maximum(count - jnp.where(headed, float(HEAD), 0.0), 0.0)
    g, p = iota((total, total), 0), iota((total, total), 1)
    lower = one((g // (2 * experts) == p // (2 * experts)) & (p < g)).astype(BF16)
    before = jnp.dot(lower, jnp.broadcast_to(beyond, (total, 128)).astype(BF16), preferred_element_type=F32)
    return beyond, before


def place_rows(table, me, core, n, experts, cap, place):
    lanes = 2 * experts * cap
    fills = jnp.concatenate([table[me, 0:experts], table[me + 1 - 2 * core, 0:experts], jnp.zeros((128 - 2 * experts, 128), F32)])
    fills = fills.T
    k, lane = iota((128, lanes), 0), iota((128, lanes), 1)
    early = lax.rem(iota((128, 128), 1), experts) < HEADED
    extra = jnp.maximum(fills - jnp.where(early, float(HEAD), 0.0), 0.0)
    rank_k = lax.rem(k + experts * core, 2 * experts)
    rank_l = lax.rem(lane // cap + experts * core, 2 * experts)
    spread = one(k == lane // cap).astype(BF16)
    earlier = one((rank_k < rank_l) & (k < 2 * experts)).astype(BF16)
    filled = jnp.dot(fills.astype(BF16), spread, preferred_element_type=F32)
    start = jnp.dot(extra.astype(BF16), earlier, preferred_element_type=F32)
    slot = lax.rem(lane, cap)
    skip = jnp.where(lax.rem(lane // cap, experts) < HEADED, HEAD, 0)
    spot = jnp.where((slot >= skip) & (slot.astype(F32) < filled), start.astype(I32) + slot - skip, -1)
    place[...] = spot[0:n]


def token_spots(expert, slot, before, chip, side, experts):
    total, tokens = before.shape[0], expert.shape[1]
    lead = []
    for c in range(expert.shape[0]):
        hit = iota((total, tokens), 0) == expert[c:c + 1]
        lead.append(jnp.sum(jnp.where(hit, before, 0.0), axis=0, keepdims=True))
    lead = jnp.concatenate(lead, axis=0).astype(I32)
    local = lax.rem(expert, experts)
    early = local < HEADED
    in_head = early & (slot >= 0) & (slot < HEAD)
    head_spot = jnp.where(in_head, ((expert // experts) * HEADED + local) * 8 + slot, -64)
    home = expert // (2 * experts)
    order = jnp.full(expert.shape, side * side - 1, I32)
    for i, (dx, dy) in enumerate(ORDER):
        came = lax.rem(chip // side + side - dy, side) * side + lax.rem(lax.rem(chip, side) + side - dx, side)
        order = jnp.where(home == came, i, order)
    skip = jnp.where(early, HEAD, 0)
    return head_spot, order, jnp.where(slot >= skip, lead + slot - skip, -1)


def set_keys(keys, spots, weight):
    tokens = weight.shape[1]
    rows = [k.astype(F32) for k in spots] + [weight]
    rows.append(jnp.zeros((128 - len(rows) * weight.shape[0], tokens), F32))
    keys[...] = jnp.concatenate(rows).T


def mix(keys, top, first, weight, add, mix_ref, base):
    tokens = keys.shape[0]

    def tile(i, carry):
        lane = (iota((tokens, 128), 1) + (i * 128 - add)).astype(F32)
        w = jnp.zeros((tokens, 128), F32)
        for c in range(top):
            w = w + jnp.where(lane == keys[:, first + c:first + c + 1], keys[:, weight + c:weight + c + 1], 0.0)
        cols = pl.ds(pl.multiple_of(i * 128, 128), 128)
        for p, part in enumerate(split3(w)):
            mix_ref[pl.ds(base + p * tokens, tokens), cols] = part
        return carry
    lax.fori_loop(0, mix_ref.shape[1] // 128, tile, 0)


def fold(v, base, tokens):
    return v[base:base + tokens] + (v[base + tokens:base + 2 * tokens] + v[base + 2 * tokens:base + 3 * tokens])


def weigh(got, mix_ref, cols):
    rows = got.shape[0] * got.shape[1]
    v = jnp.dot(mix_ref[...], got[:, :, cols].reshape(rows, COLS), preferred_element_type=F32)
    return fold(v, 0, mix_ref.shape[0] // 3)


def main_kernel(n, fill, fill_v, expert_t, slot_t, weight_t, x, w_gate, w_up, w_down, own, other, table, branch, total,
                x_buf, gate_buf, up_buf, down_buf, hidden, mask, rows, theirs, head, head_in, note, place, keys,
                head_mix, mix_a, mix_b, pack_a, pack_b, got_a, got_b,
                load_sem, x_sem, own_sem, theirs_sem, pair_send, pair_recv, head_send, head_recv, note_send, note_recv, send_sem, recv_sem):
    me = lax.axis_index("ep")
    core = me & 1
    chip = lax.shift_right_logical(me, 1)
    chips = n // 2
    side = math.isqrt(chips)
    _, _, experts, cap, width = x.shape
    sources = n
    ffn = w_gate.shape[2]
    half = width // 2
    top, tokens = expert_t.shape
    cut = got_a.shape[1]
    rest = got_b.shape[1]
    barrier = pltpu.get_barrier_semaphore()

    def load_x(e, slot, h):
        return pltpu.make_async_copy(x.at[:, (core + 1 + h) & 1, e], x_buf.at[slot, h], x_sem.at[slot, h])

    def load_w(e, slot):
        return (
            pltpu.make_async_copy(w_gate.at[e], gate_buf.at[slot], load_sem.at[0, slot]),
            pltpu.make_async_copy(w_up.at[e], up_buf.at[slot], load_sem.at[1, slot]),
            pltpu.make_async_copy(w_down.at[e], down_buf.at[slot], load_sem.at[2, slot]),
        )

    def loads(e, slot):
        return (load_x(e, slot, 0),) + load_w(e, slot) + (load_x(e, slot, 1),)

    for copy in loads(0, 0):
        copy.start()

    def greet(k, carry):
        pl.semaphore_signal(barrier, inc=1, device_id={"ep": (me + k) & (n - 1)}, device_id_type=MESH)
        return carry
    lax.fori_loop(1, n, greet, 0)

    beyond, before = needs(expert_t[...], slot_t[...], n * experts, experts)
    note[...] = jnp.zeros_like(note)
    note[0:experts, 0:sources] = fill_v[...].astype(F32)
    note[experts:experts + 1, :] = jnp.max(before + beyond, axis=0, keepdims=True)
    def own_copy(e):
        return pltpu.make_async_copy(rows.at[1, e], own.at[e], own_sem.at[e])

    def pair_copy(e):
        return pltpu.make_async_remote_copy(
            src_ref=rows.at[0, e], dst_ref=theirs.at[e], send_sem=pair_send.at[e], recv_sem=pair_recv.at[e],
            device_id={"ep": me + 1 - 2 * core}, device_id_type=MESH)

    def block(t, carry):
        e = lax.shift_right_logical(t, 1)
        h = t & 1
        slot = e & 1
        to_core = (core + 1 + h) & 1

        @pl.when((h == 0) & (e + 1 < experts))
        def _():
            for copy in loads(e + 1, 1 - slot):
                copy.start()

        for j in range(chips):
            mask[pl.ds(j * cap, cap), :] = one(iota((cap, 128), 0) < fill[e, 2 * j + to_core])
        weights = load_w(e, slot)
        load_x(e, slot, h).wait()

        @pl.when(h == 0)
        def _():
            weights[0].wait()
            weights[1].wait()

        def up(k, carry):
            cols = pl.ds(pl.multiple_of(k * COLS, COLS), COLS)
            act = x_buf[slot, h].reshape(chips * cap, width)
            a = jnp.dot(act, gate_buf[slot, :, cols], preferred_element_type=F32)
            b = jnp.dot(act, up_buf[slot, :, cols], preferred_element_type=F32)
            hidden[:, cols] = (a * jax.nn.sigmoid(a) * b).astype(BF16)
            return carry
        lax.fori_loop(0, ffn // COLS, up, 0, unroll=True)

        @pl.when(h == 0)
        def _():
            weights[2].wait()

        def down(k, carry):
            live = jnp.concatenate([mask[...]] * (COLS // 128), axis=1) > 0.5
            tops = []
            for part in range(2):
                cols = pl.ds(pl.multiple_of(part * half + k * COLS, COLS), COLS)
                y = jnp.dot(hidden[...], down_buf[slot, :, cols], preferred_element_type=F32)
                y = jnp.where(live, y, 0.0)
                rows[h, e, :, :, cols] = y.astype(BF16).reshape(chips, cap, COLS)
                tops.append(y.reshape(chips, cap, COLS)[:, :8])
            first = iota((chips, 8, COLS), 1) < HEAD
            shifted = pltpu.roll(tops[1], HEAD, 1)
            cols = pl.ds(pl.multiple_of(k * COLS, COLS), COLS)
            head[h, e, :, :, cols] = jnp.where(first, tops[0], shifted).astype(BF16)
            return carry
        lax.fori_loop(0, half // COLS, down, 0, unroll=True)

        @pl.when(t == 0)
        def _():
            pl.semaphore_wait(barrier, n - 1)

        def push(j):
            pltpu.make_async_remote_copy(
                src_ref=head.at[h, e, j], dst_ref=head_in.at[me * HEADED + e], send_sem=head_send.at[h],
                recv_sem=head_recv, device_id={"ep": 2 * j + to_core}, device_id_type=MESH).start()

        @pl.when(e < HEADED)
        def _():
            def away(i, carry):
                push(step_to(chip, side, i))
                return carry
            lax.fori_loop(0, chips - 1, away, 0)

        @pl.when((h == 0) & (e < HEADED))
        def _():
            push(chip)

        @pl.when((h == 1) & (e < HEADED))
        def _():
            pltpu.make_async_copy(head.at[1, e, chip], head_in.at[me * HEADED + e], head_recv).start()

        @pl.when(h == 0)
        def _():
            pair_copy(e).start()

        @pl.when(h == 1)
        def _():
            own_copy(e).start()

        @pl.when(t == 0)
        def _():
            def tell(k, carry):
                pltpu.make_async_remote_copy(
                    src_ref=note, dst_ref=table.at[me], send_sem=note_send, recv_sem=note_recv,
                    device_id={"ep": (me + k) & (n - 1)}, device_id_type=MESH).start()
                return carry
            lax.fori_loop(1, n, tell, 0)
            table[me] = note[...]
        return carry
    lax.fori_loop(0, 2 * experts, block, 0)

    noted = table.at[pl.ds(0, n - 1)]
    pltpu.make_async_copy(noted, noted, note_recv).wait()
    pltpu.make_async_copy(noted, noted, note_send).wait()
    place_rows(table, me, core, n, experts, cap, place)
    for e in range(experts):
        pair_copy(e).wait_recv()

    def chunk(j):
        lanes = 2 * experts * cap
        pick = one(iota((cut + rest, lanes), 0) == place[pl.ds(2 * j + core, 1), :]).astype(BF16)
        near = rows[1, :, pl.ds(j, 1)].reshape(experts * cap, width)
        far = theirs[:, pl.ds(j, 1)].reshape(experts * cap, width)
        both = jnp.concatenate([near, far], axis=0)
        return jnp.dot(pick, both, preferred_element_type=F32).astype(BF16)

    def send(p, i, j):
        return pltpu.make_async_remote_copy(
            src_ref=(pack_a, pack_b)[p].at[i], dst_ref=(got_a, got_b)[p].at[i], send_sem=send_sem.at[p],
            recv_sem=recv_sem.at[p], device_id={"ep": 2 * j + core}, device_id_type=MESH)

    def push_first(i, carry):
        j = step_to(chip, side, i)
        block = chunk(j)
        pack_a[i] = block[:cut]
        pack_b[i] = block[cut:]
        send(0, i, j).start()
        return carry
    lax.fori_loop(0, chips - 1, push_first, 0)

    def push_rest(i, carry):
        send(1, i, step_to(chip, side, i)).start()
        return carry
    lax.fori_loop(0, chips - 1, push_rest, 0)
    block = chunk(chip)
    got_a[chips - 1] = block[:cut]
    got_b[chips - 1] = block[cut:]

    theirs_copy = pltpu.make_async_copy(theirs, other, theirs_sem)
    theirs_copy.start()
    most = jnp.max(jnp.max(table[...], axis=0)[experts:experts + 1, :])
    index = (most > float(cut + rest)).astype(I32)
    for more in MORE:
        index = index + (most > float(cut + rest + more)).astype(I32)
    branch[0, 0] = index

    _, before = needs(expert_t[...], slot_t[...], n * experts, experts)
    head_spot, order, spot = token_spots(expert_t[...], slot_t[...], before, chip, side, experts)
    key_a = jnp.where((spot >= 0) & (spot < cut), order * cut + spot, -64)
    key_b = jnp.where((spot >= cut) & (spot < cut + rest), order * rest + spot - cut, -64)
    set_keys(keys, (head_spot, key_a, key_b), weight_t[...])
    mix(keys, top, 0, 3 * top, 0, head_mix.at[pl.ds(0, 3 * tokens)], 0)
    mix(keys, top, 0, 3 * top, HEAD, head_mix.at[pl.ds(3 * tokens, 3 * tokens)], 0)
    mix(keys, top, top, 3 * top, 0, mix_a, 0)
    mix(keys, top, 2 * top, 3 * top, 0, mix_b, 0)
    pltpu.make_async_copy(head_in, head_in, head_recv).wait()

    def head_cols(i, carry):
        cols = pl.ds(pl.multiple_of(i * COLS, COLS), COLS)
        head_rows = head_in.shape[0] * head_in.shape[1]
        v = jnp.dot(head_mix[...], head_in[:, :, cols].reshape(head_rows, COLS), preferred_element_type=F32)
        total[:, cols] = fold(v, 0, tokens)
        total[:, pl.ds(pl.multiple_of(half + i * COLS, COLS), COLS)] = fold(v, 3 * tokens, tokens)
        return carry
    lax.fori_loop(0, half // COLS, head_cols, 0)

    for p, (got, mix_ref) in enumerate(((got_a, mix_a), (got_b, mix_b))):
        taken = got.at[pl.ds(0, chips - 1)]
        pltpu.make_async_copy(taken, taken, recv_sem.at[p]).wait()

        def some_cols(i, carry):
            cols = pl.ds(pl.multiple_of(i * COLS, COLS), COLS)
            total[:, cols] += weigh(got, mix_ref, cols)
            return carry
        lax.fori_loop(0, width // COLS, some_cols, 0, unroll=p == 1)

    for p, sent in enumerate((pack_a, pack_b)):
        pltpu.make_async_copy(sent, sent, send_sem.at[p]).wait()
    for e in range(experts):
        own_copy(e).wait()
        pair_copy(e).wait_send()
    for h in range(2):
        sent = head.at[h, pl.ds(0, HEADED), pl.ds(0, chips - h)]
        pltpu.make_async_copy(sent, sent, head_send.at[h]).wait()
    theirs_copy.wait()


def split3(w):
    hi = jnp.minimum(w, 3.3895313892515355e38).astype(BF16)
    rest = w - hi.astype(F32)
    mid = rest.astype(BF16)
    low = (rest - mid.astype(F32)).astype(BF16)
    return hi, mid, low


def more_kernel(n, room, table, expert_t, slot_t, weight_t, total, own, other, out,
                src, pack, got, mix_ref, place, keys, load_sem, send_sem, recv_sem):
    me = lax.axis_index("ep")
    core = me & 1
    chip = lax.shift_right_logical(me, 1)
    chips = n // 2
    side = math.isqrt(chips)
    experts, _, cap, width = own.shape
    top, tokens = expert_t.shape
    barrier = pltpu.get_barrier_semaphore()

    def greet(i, carry):
        pl.semaphore_signal(barrier, inc=1, device_id={"ep": 2 * step_to(chip, side, i) + core}, device_id_type=MESH)
        return carry
    lax.fori_loop(0, chips - 1, greet, 0)

    def load(i, j):
        return (pltpu.make_async_copy(own.at[:, j], src.at[i, 0], load_sem.at[i, 0]),
                pltpu.make_async_copy(other.at[:, j], src.at[i, 1], load_sem.at[i, 1]))

    def load_to(i, carry):
        for copy in load(i, step_to(chip, side, i)):
            copy.start()
        return carry
    lax.fori_loop(0, chips - 1, load_to, 0)
    for copy in load(chips - 1, chip):
        copy.start()
    place_rows(table, me, core, n, experts, cap, place)

    def chunk(i, j):
        for copy in load(i, j):
            copy.wait()
        lanes = 2 * experts * cap
        pick = one(iota((room, lanes), 0) + ROOM == place[pl.ds(2 * j + core, 1), :]).astype(BF16)
        return jnp.dot(pick, src[i].reshape(lanes, width), preferred_element_type=F32).astype(BF16)

    def send(i, j):
        return pltpu.make_async_remote_copy(
            src_ref=pack.at[i], dst_ref=got.at[i], send_sem=send_sem, recv_sem=recv_sem,
            device_id={"ep": 2 * j + core}, device_id_type=MESH)

    pl.semaphore_wait(barrier, chips - 1)

    def push(i, carry):
        j = step_to(chip, side, i)
        pack[i] = chunk(i, j)
        send(i, j).start()
        return carry
    lax.fori_loop(0, chips - 1, push, 0)
    got[chips - 1] = chunk(chips - 1, chip)

    _, before = needs(expert_t[...], slot_t[...], n * experts, experts)
    _, order, spot = token_spots(expert_t[...], slot_t[...], before, chip, side, experts)
    key = jnp.where((spot >= ROOM) & (spot < ROOM + room), order * room + spot - ROOM, -64)
    set_keys(keys, (key,), weight_t[...])
    mix(keys, top, 0, top, 0, mix_ref, 0)

    taken = got.at[pl.ds(0, chips - 1)]
    pltpu.make_async_copy(taken, taken, recv_sem).wait()

    def cols_of(i, carry):
        cols = pl.ds(pl.multiple_of(i * COLS, COLS), COLS)
        out[:, cols] = total[:, cols] + weigh(got, mix_ref, cols)
        return carry
    lax.fori_loop(0, width // COLS, cols_of, 0)
    pltpu.make_async_copy(pack, pack, send_sem).wait()


def solution(mesh):
    n = mesh.shape["ep"]
    chips = n // 2

    def step(dispatched, w_gate, w_up, w_down, fill_count, slot_index, expert_id, gate_weight):
        sources, experts, cap, width = dispatched.shape
        ffn = w_gate.shape[2]
        tokens, top = slot_index.shape
        most = 2 * (HEADED * (cap - HEAD) + (experts - HEADED) * cap)
        cut = -(-ROOM // 16) * 8
        any_spec = pl.BlockSpec(memory_space=pl.ANY)
        vmem_spec = pl.BlockSpec(memory_space=pltpu.VMEM)
        smem_spec = pl.BlockSpec(memory_space=pltpu.SMEM)
        shape = jax.ShapeDtypeStruct
        vmem = pltpu.VMEM
        dma = pltpu.SemaphoreType.DMA
        fill_t, expert_t, slot_t, weight_t = fill_count.T, expert_id.T, slot_index.T, gate_weight.T
        own, other, table, branch, total = pl.pallas_call(
            functools.partial(main_kernel, n),
            name="main",
            out_shape=(
                shape((experts, chips, cap, width), BF16),
                shape((experts, chips, cap, width), BF16),
                shape((n, 8, 128), F32),
                shape((1, 1), I32),
                shape((tokens, width), F32),
            ),
            in_specs=[smem_spec] + [vmem_spec] * 4 + [any_spec] * 4,
            out_specs=(any_spec,) * 2 + (vmem_spec, smem_spec, vmem_spec),
            scratch_shapes=[
                vmem((2, 2, chips, cap, width), BF16),
                vmem((2, width, ffn), BF16),
                vmem((2, width, ffn), BF16),
                vmem((2, ffn, width), BF16),
                vmem((chips * cap, ffn), BF16),
                vmem((chips * cap, 128), F32),
                vmem((2, experts, chips, cap, width), BF16),
                vmem((experts, chips, cap, width), BF16),
                vmem((2, experts, chips, 8, width // 2), BF16),
                vmem((n * HEADED, 8, width // 2), BF16),
                vmem((8, 128), F32),
                vmem((n, 2 * experts * cap), I32),
                vmem((tokens, 128), F32),
                vmem((6 * tokens, n * HEADED * 8), BF16),
                vmem((3 * tokens, chips * cut), BF16),
                vmem((3 * tokens, chips * (ROOM - cut)), BF16),
                vmem((chips - 1, cut, width), BF16),
                vmem((chips - 1, ROOM - cut, width), BF16),
                vmem((chips, cut, width), BF16),
                vmem((chips, ROOM - cut, width), BF16),
                dma((3, 2)), dma((2, 2)), dma((experts,)), dma, dma((experts,)), dma((experts,)), dma((2,)), dma, dma, dma, dma((2,)), dma((2,)),
            ],
            compiler_params=pltpu.CompilerParams(collective_id=0, has_side_effects=True, vmem_limit_bytes=GRANT),
        )(fill_t, fill_t, expert_t, slot_t, weight_t, dispatched.reshape(chips, 2, experts, cap, width), w_gate, w_up, w_down)

        def more(room, index):
            result = pl.pallas_call(
                functools.partial(more_kernel, n, room),
                name="more%d" % room,
                out_shape=shape((tokens, width), F32),
                in_specs=[vmem_spec] * 5 + [any_spec] * 2,
                out_specs=vmem_spec,
                scratch_shapes=[
                    vmem((chips, 2, experts, cap, width), BF16),
                    vmem((chips - 1, room, width), BF16),
                    vmem((chips, room, width), BF16),
                    vmem((3 * tokens, chips * room), BF16),
                    vmem((n, 2 * experts * cap), I32),
                    vmem((tokens, 128), F32),
                    dma((chips, 2)), dma, dma,
                ],
                compiler_params=pltpu.CompilerParams(collective_id=1 + index, has_side_effects=True, vmem_limit_bytes=GRANT),
            )(table, expert_t, slot_t, weight_t, total, own, other)
            return result.astype(BF16)

        rooms = MORE + (most - ROOM,)
        return lax.switch(branch[0, 0], [lambda: total.astype(BF16)] + [functools.partial(more, r, i) for i, r in enumerate(rooms)])

    token_spec = P(("dp", "ep"))
    in_specs = (P("dp", "ep"), P("ep"), P("ep"), P("ep"), P("dp", "ep"), token_spec, token_spec, token_spec)
    return jax.shard_map(step, mesh=mesh, in_specs=in_specs, out_specs=token_spec, check_vma=False)
```

```python
import functools
import math

import jax
import jax.numpy as jnp
from jax import lax
from jax.experimental import pallas as pl
from jax.experimental.pallas import tpu as pltpu
from jax.sharding import PartitionSpec as P

MESH = pl.DeviceIdType.MESH
BF16, F32, I32 = jnp.bfloat16, jnp.float32, jnp.int32
HEAD = 4
HEADED = 3
COLS = 256
UNROLL = 3
ROOM = 48
MORE = (8, 16, 24, 40)
GRANT = 64 * 1024 * 1024 - 65536
ORDER = ((2, 2), (2, 1), (2, 3), (1, 2), (3, 2), (2, 0), (0, 2), (1, 1), (3, 3), (1, 3), (3, 1), (1, 0), (3, 0), (0, 1), (0, 3))
STEP_X = sum(x << (2 * i) for i, (x, y) in enumerate(ORDER))
STEP_Y = sum(y << (2 * i) for i, (x, y) in enumerate(ORDER))


def step_to(chip, side, i):
    dx = lax.shift_right_logical(jnp.int32(STEP_X), 2 * i) & 3
    dy = lax.shift_right_logical(jnp.int32(STEP_Y), 2 * i) & 3
    return ((chip + dy * side) & (side * side - side)) + ((chip + dx) & (side - 1))


def iota(shape, dim):
    return lax.broadcasted_iota(I32, shape, dim)


def low(v, m):
    return v & (m - 1)


def high(v, m):
    return lax.shift_right_logical(v, m.bit_length() - 1)


def one(cond):
    return jnp.where(cond, 1.0, 0.0)


def needs(expert_t, slot_t, total, experts):
    tokens = expert_t.shape[1]
    hit = jnp.zeros((total, tokens), F32)
    for c in range(expert_t.shape[0]):
        hit = hit + one((iota((total, tokens), 0) == expert_t[c:c + 1]) & (slot_t[c:c + 1] >= 0))
    count = jnp.sum(hit, axis=1, keepdims=True)
    headed = low(iota((total, 1), 0), experts) < HEADED
    beyond = jnp.maximum(count - jnp.where(headed, float(HEAD), 0.0), 0.0)
    g, p = iota((total, total), 0), iota((total, total), 1)
    lower = one((high(g, 2 * experts) == high(p, 2 * experts)) & (p < g)).astype(BF16)
    before = jnp.dot(lower, jnp.broadcast_to(beyond, (total, 128)).astype(BF16), preferred_element_type=F32)
    return beyond, before


def place_rows(table, me, core, n, experts, cap, place):
    lanes = 2 * experts * cap
    fills = jnp.concatenate([table[me, 0:experts], table[me + 1 - 2 * core, 0:experts], jnp.zeros((128 - 2 * experts, 128), F32)])
    fills = fills.T
    k, lane = iota((128, lanes), 0), iota((128, lanes), 1)
    early = low(iota((128, 128), 1), experts) < HEADED
    extra = jnp.maximum(fills - jnp.where(early, float(HEAD), 0.0), 0.0)
    rank_k = low(k + experts * core, 2 * experts)
    rank_l = low(high(lane, cap) + experts * core, 2 * experts)
    spread = one(k == high(lane, cap)).astype(BF16)
    earlier = one((rank_k < rank_l) & (k < 2 * experts)).astype(BF16)
    filled = jnp.dot(fills.astype(BF16), spread, preferred_element_type=F32)
    start = jnp.dot(extra.astype(BF16), earlier, preferred_element_type=F32)
    slot = low(lane, cap)
    skip = jnp.where(low(high(lane, cap), experts) < HEADED, HEAD, 0)
    spot = jnp.where((slot >= skip) & (slot.astype(F32) < filled), start.astype(I32) + slot - skip, -1)
    place[...] = spot[0:n]


def token_spots(expert, slot, before, chip, side, experts):
    total, tokens = before.shape[0], expert.shape[1]
    lead = []
    for c in range(expert.shape[0]):
        hit = iota((total, tokens), 0) == expert[c:c + 1]
        lead.append(jnp.sum(jnp.where(hit, before, 0.0), axis=0, keepdims=True))
    lead = jnp.concatenate(lead, axis=0).astype(I32)
    local = low(expert, experts)
    early = local < HEADED
    in_head = early & (slot >= 0) & (slot < HEAD)
    head_spot = jnp.where(in_head, (high(expert, experts) * HEADED + local) * 8 + slot, -64)
    home = high(expert, 2 * experts)
    order = jnp.full(expert.shape, side * side - 1, I32)
    for i, (dx, dy) in enumerate(ORDER):
        came = lax.rem(chip // side + side - dy, side) * side + lax.rem(lax.rem(chip, side) + side - dx, side)
        order = jnp.where(home == came, i, order)
    skip = jnp.where(early, HEAD, 0)
    return head_spot, order, jnp.where(slot >= skip, lead + slot - skip, -1)


def set_keys(keys, spots, weight):
    tokens = weight.shape[1]
    rows = [k.astype(F32) for k in spots] + [weight]
    rows.append(jnp.zeros((128 - len(rows) * weight.shape[0], tokens), F32))
    keys[...] = jnp.concatenate(rows).T


def mix(keys, top, first, weight, add, mix_ref, base):
    tokens = keys.shape[0]

    def tile(i, carry):
        lane = (iota((tokens, 128), 1) + (i * 128 - add)).astype(F32)
        w = jnp.zeros((tokens, 128), F32)
        for c in range(top):
            w = w + jnp.where(lane == keys[:, first + c:first + c + 1], keys[:, weight + c:weight + c + 1], 0.0)
        cols = pl.ds(pl.multiple_of(i * 128, 128), 128)
        for p, part in enumerate(split3(w)):
            mix_ref[pl.ds(base + p * tokens, tokens), cols] = part
        return carry
    lax.fori_loop(0, mix_ref.shape[1] // 128, tile, 0)


def fold(v, base, tokens):
    return v[base:base + tokens] + (v[base + tokens:base + 2 * tokens] + v[base + 2 * tokens:base + 3 * tokens])


def weigh(got, mix_ref, cols):
    rows = got.shape[0] * got.shape[1]
    v = jnp.dot(mix_ref[...], got[:, :, cols].reshape(rows, COLS), preferred_element_type=F32)
    return fold(v, 0, mix_ref.shape[0] // 3)


def main_kernel(n, fill, fill_v, expert_t, slot_t, weight_t, x, w_gate, w_up, w_down, own, other, table, branch, total,
                x_buf, gate_buf, up_buf, down_buf, hidden_a, hidden_b, mask, rows, theirs, head, head_in, note, place, keys,
                head_mix, mix_a, mix_b, pack_a, pack_b, got_a, got_b,
                load_sem, x_sem, piece_sem, own_sem, theirs_sem, pair_send, pair_recv, head_send, head_recv, note_send, note_recv, send_sem, recv_sem):
    me = lax.axis_index("ep")
    core = me & 1
    chip = lax.shift_right_logical(me, 1)
    chips = n // 2
    side = math.isqrt(chips)
    _, _, experts, cap, width = x.shape
    sources = n
    ffn = w_gate.shape[2]
    half = width // 2
    top, tokens = expert_t.shape
    cut = got_a.shape[1]
    rest = got_b.shape[1]
    hidden = (hidden_a, hidden_b)
    barrier = pltpu.get_barrier_semaphore()

    def load_x(e, h):
        return pltpu.make_async_copy(x.at[:, (core + 1 + h) & 1, e], x_buf.at[e & 1, h], x_sem.at[e & 1, h])

    def load_in(e):
        return (pltpu.make_async_copy(w_gate.at[e], gate_buf.at[e & 1], load_sem.at[0, e & 1]),
                pltpu.make_async_copy(w_up.at[e], up_buf.at[e & 1], load_sem.at[1, e & 1]))

    def load_down(e):
        return pltpu.make_async_copy(w_down.at[e], down_buf.at[e & 1], load_sem.at[2, e & 1])

    def load_piece(k):
        cols = pl.ds(k * COLS, COLS)
        return (pltpu.make_async_copy(w_gate.at[0, :, cols], gate_buf.at[0, :, cols], piece_sem.at[0, k]),
                pltpu.make_async_copy(w_up.at[0, :, cols], up_buf.at[0, :, cols], piece_sem.at[1, k]))

    pieces = ffn // COLS
    load_x(0, 0).start()
    for k in range(pieces):
        for copy in load_piece(k):
            copy.start()
    load_down(0).start()
    load_x(0, 1).start()

    def greet(k, carry):
        pl.semaphore_signal(barrier, inc=1, device_id={"ep": (me + k) & (n - 1)}, device_id_type=MESH)
        return carry
    lax.fori_loop(1, n, greet, 0, unroll=8)

    beyond, before = needs(expert_t[...], slot_t[...], n * experts, experts)
    note[...] = jnp.zeros_like(note)
    note[0:experts, 0:sources] = fill_v[...].astype(F32)
    note[experts:experts + 1, :] = jnp.max(before + beyond, axis=0, keepdims=True)
    def set_mask(t, carry):
        for j in range(chips):
            full = fill[lax.shift_right_logical(t, 1), 2 * j + ((core + 1 + t) & 1)]
            mask[t, pl.ds(j * cap, cap), :] = one(iota((cap, 128), 0) < full)
        return carry
    lax.fori_loop(0, 2 * experts, set_mask, 0)

    def own_copy(e):
        return pltpu.make_async_copy(rows.at[1, e], own.at[e], own_sem.at[e])

    def pair_copy(e):
        return pltpu.make_async_remote_copy(
            src_ref=rows.at[0, e], dst_ref=theirs.at[e], send_sem=pair_send.at[e], recv_sem=pair_recv.at[e],
            device_id={"ep": me + 1 - 2 * core}, device_id_type=MESH)

    def up(e, h, k):
        cols = pl.ds(k * COLS, COLS)
        act = x_buf[e & 1, h].reshape(chips * cap, width)
        a = jnp.dot(act, gate_buf[e & 1, :, cols], preferred_element_type=F32)
        b = jnp.dot(act, up_buf[e & 1, :, cols], preferred_element_type=F32)
        hidden[h][:, cols] = (a * jax.nn.sigmoid(a) * b).astype(BF16)

    def down(e, h, k):
        live = jnp.concatenate([mask[2 * e + h]] * (COLS // 128), axis=1) > 0.5
        tops = []
        for part in range(2):
            cols = pl.ds(part * half + k * COLS, COLS)
            y = jnp.dot(hidden[h][...], down_buf[e & 1, :, cols], preferred_element_type=F32)
            y = jnp.where(live, y, 0.0)
            rows[h, e, :, :, cols] = y.astype(BF16).reshape(chips, cap, COLS)
            tops.append(y.reshape(chips, cap, COLS)[:, :8])
        first = iota((chips, 8, COLS), 1) < HEAD
        shifted = pltpu.roll(tops[1], HEAD, 1)
        head[h, e, :, :, pl.ds(k * COLS, COLS)] = jnp.where(first, tops[0], shifted).astype(BF16)

    outs = half // COLS

    def both(e_up, h_up, e_down, h_down):
        for k in range(max(pieces, outs)):
            if k < pieces:
                up(e_up, h_up, k)
            if k < outs:
                down(e_down, h_down, k)

    def push(e, h, j):
        pltpu.make_async_remote_copy(
            src_ref=head.at[h, e, j], dst_ref=head_in.at[me * HEADED + e], send_sem=head_send.at[h],
            recv_sem=head_recv, device_id={"ep": 2 * j + ((core + 1 + h) & 1)}, device_id_type=MESH).start()

    def push_all(e, h):
        def away(i, carry):
            push(e, h, step_to(chip, side, i))
            return carry
        lax.fori_loop(0, chips - 1, away, 0, unroll=True)

    load_x(0, 0).wait()
    for k in range(pieces):
        for copy in load_piece(k):
            copy.wait()
        if k == pieces - 1:
            for copy in load_in(1) + (load_x(1, 0), load_x(1, 1), load_down(1)):
                copy.start()
        up(0, 0, k)

    def expert(e, carry):
        @pl.when((e > 0) & (e + 1 < experts))
        def _():
            load_down(e + 1).start()

        load_x(e, 1).wait()
        load_down(e).wait()
        for k in range(outs):
            down(e, 0, k)

        @pl.when(e == 0)
        def _():
            pl.semaphore_wait(barrier, n - 1)

        pair_copy(e).start()

        @pl.when(e < HEADED)
        def _():
            push_all(e, 0)
            push(e, 0, chip)

        @pl.when(e == 0)
        def _():
            def tell(k, carry):
                pltpu.make_async_remote_copy(
                    src_ref=note, dst_ref=table.at[me], send_sem=note_send, recv_sem=note_recv,
                    device_id={"ep": (me + k) & (n - 1)}, device_id_type=MESH).start()
                return carry
            lax.fori_loop(1, n, tell, 0, unroll=8)
            table[me] = note[...]

        for k in range(pieces):
            up(e, 1, k)

        @pl.when(e + 2 < experts)
        def _():
            for copy in load_in(e + 2) + (load_x(e + 2, 0), load_x(e + 2, 1)):
                copy.start()

        for k in range(outs):
            down(e, 1, k)
        own_copy(e).start()

        @pl.when(e < HEADED)
        def _():
            push_all(e, 1)
            pltpu.make_async_copy(head.at[1, e, chip], head_in.at[me * HEADED + e], head_recv).start()

        @pl.when(e + 1 < experts)
        def _():
            load_x(e + 1, 0).wait()
            for copy in load_in(e + 1):
                copy.wait()
            for k in range(pieces):
                up(e + 1, 0, k)
        return carry
    lax.fori_loop(0, experts, expert, 0)

    noted = table.at[pl.ds(0, n - 1)]
    pltpu.make_async_copy(noted, noted, note_recv).wait()
    pltpu.make_async_copy(noted, noted, note_send).wait()
    place_rows(table, me, core, n, experts, cap, place)
    for e in range(experts):
        pair_copy(e).wait_recv()

    def chunk(j):
        lanes = 2 * experts * cap
        pick = one(iota((cut + rest, lanes), 0) == place[pl.ds(2 * j + core, 1), :]).astype(BF16)
        near = rows[1, :, pl.ds(j, 1)].reshape(experts * cap, width)
        far = theirs[:, pl.ds(j, 1)].reshape(experts * cap, width)
        both = jnp.concatenate([near, far], axis=0)
        return jnp.dot(pick, both, preferred_element_type=F32).astype(BF16)

    def send(p, i, j):
        return pltpu.make_async_remote_copy(
            src_ref=(pack_a, pack_b)[p].at[i], dst_ref=(got_a, got_b)[p].at[i], send_sem=send_sem.at[p],
            recv_sem=recv_sem.at[p], device_id={"ep": 2 * j + core}, device_id_type=MESH)

    def push_first(i, carry):
        j = step_to(chip, side, i)
        block = chunk(j)
        pack_a[i] = block[:cut]
        pack_b[i] = block[cut:]
        send(0, i, j).start()
        return carry
    lax.fori_loop(0, chips - 1, push_first, 0, unroll=UNROLL)

    def push_rest(i, carry):
        send(1, i, step_to(chip, side, i)).start()
        return carry
    lax.fori_loop(0, chips - 1, push_rest, 0)
    block = chunk(chip)
    got_a[chips - 1] = block[:cut]
    got_b[chips - 1] = block[cut:]

    theirs_copy = pltpu.make_async_copy(theirs, other, theirs_sem)
    theirs_copy.start()
    most = jnp.max(jnp.max(table[...], axis=0)[experts:experts + 1, :])
    index = (most > float(cut + rest)).astype(I32)
    for more in MORE:
        index = index + (most > float(cut + rest + more)).astype(I32)
    branch[0, 0] = index

    _, before = needs(expert_t[...], slot_t[...], n * experts, experts)
    head_spot, order, spot = token_spots(expert_t[...], slot_t[...], before, chip, side, experts)
    key_a = jnp.where((spot >= 0) & (spot < cut), order * cut + spot, -64)
    key_b = jnp.where((spot >= cut) & (spot < cut + rest), order * rest + spot - cut, -64)
    set_keys(keys, (head_spot, key_a, key_b), weight_t[...])
    mix(keys, top, 0, 3 * top, 0, head_mix.at[pl.ds(0, 3 * tokens)], 0)
    mix(keys, top, 0, 3 * top, HEAD, head_mix.at[pl.ds(3 * tokens, 3 * tokens)], 0)
    mix(keys, top, top, 3 * top, 0, mix_a, 0)
    mix(keys, top, 2 * top, 3 * top, 0, mix_b, 0)
    pltpu.make_async_copy(head_in, head_in, head_recv).wait()

    def head_cols(i, carry):
        cols = pl.ds(pl.multiple_of(i * COLS, COLS), COLS)
        head_rows = head_in.shape[0] * head_in.shape[1]
        v = jnp.dot(head_mix[...], head_in[:, :, cols].reshape(head_rows, COLS), preferred_element_type=F32)
        total[:, cols] = fold(v, 0, tokens)
        total[:, pl.ds(pl.multiple_of(half + i * COLS, COLS), COLS)] = fold(v, 3 * tokens, tokens)
        return carry
    lax.fori_loop(0, half // COLS, head_cols, 0)

    for p, (got, mix_ref) in enumerate(((got_a, mix_a), (got_b, mix_b))):
        taken = got.at[pl.ds(0, chips - 1)]
        pltpu.make_async_copy(taken, taken, recv_sem.at[p]).wait()

        def some_cols(i, carry):
            cols = pl.ds(pl.multiple_of(i * COLS, COLS), COLS)
            total[:, cols] += weigh(got, mix_ref, cols)
            return carry
        lax.fori_loop(0, width // COLS, some_cols, 0, unroll=p == 1)

    for p, sent in enumerate((pack_a, pack_b)):
        pltpu.make_async_copy(sent, sent, send_sem.at[p]).wait()
    for e in range(experts):
        own_copy(e).wait()
        pair_copy(e).wait_send()
    for h in range(2):
        sent = head.at[h, pl.ds(0, HEADED), pl.ds(0, chips - h)]
        pltpu.make_async_copy(sent, sent, head_send.at[h]).wait()
    theirs_copy.wait()


def split3(w):
    hi = jnp.minimum(w, 3.3895313892515355e38).astype(BF16)
    rest = w - hi.astype(F32)
    mid = rest.astype(BF16)
    low = (rest - mid.astype(F32)).astype(BF16)
    return hi, mid, low


def more_kernel(n, room, table, expert_t, slot_t, weight_t, total, own, other, out,
                src, pack, got, mix_ref, place, keys, load_sem, send_sem, recv_sem):
    me = lax.axis_index("ep")
    core = me & 1
    chip = lax.shift_right_logical(me, 1)
    chips = n // 2
    side = math.isqrt(chips)
    experts, _, cap, width = own.shape
    top, tokens = expert_t.shape
    barrier = pltpu.get_barrier_semaphore()

    def greet(i, carry):
        pl.semaphore_signal(barrier, inc=1, device_id={"ep": 2 * step_to(chip, side, i) + core}, device_id_type=MESH)
        return carry
    lax.fori_loop(0, chips - 1, greet, 0)

    def load(i, j):
        return (pltpu.make_async_copy(own.at[:, j], src.at[i, 0], load_sem.at[i, 0]),
                pltpu.make_async_copy(other.at[:, j], src.at[i, 1], load_sem.at[i, 1]))

    def load_to(i, carry):
        for copy in load(i, step_to(chip, side, i)):
            copy.start()
        return carry
    lax.fori_loop(0, chips - 1, load_to, 0)
    for copy in load(chips - 1, chip):
        copy.start()
    place_rows(table, me, core, n, experts, cap, place)

    def chunk(i, j):
        for copy in load(i, j):
            copy.wait()
        lanes = 2 * experts * cap
        pick = one(iota((room, lanes), 0) + ROOM == place[pl.ds(2 * j + core, 1), :]).astype(BF16)
        return jnp.dot(pick, src[i].reshape(lanes, width), preferred_element_type=F32).astype(BF16)

    def send(i, j):
        return pltpu.make_async_remote_copy(
            src_ref=pack.at[i], dst_ref=got.at[i], send_sem=send_sem, recv_sem=recv_sem,
            device_id={"ep": 2 * j + core}, device_id_type=MESH)

    pl.semaphore_wait(barrier, chips - 1)

    def push(i, carry):
        j = step_to(chip, side, i)
        pack[i] = chunk(i, j)
        send(i, j).start()
        return carry
    lax.fori_loop(0, chips - 1, push, 0)
    got[chips - 1] = chunk(chips - 1, chip)

    _, before = needs(expert_t[...], slot_t[...], n * experts, experts)
    _, order, spot = token_spots(expert_t[...], slot_t[...], before, chip, side, experts)
    key = jnp.where((spot >= ROOM) & (spot < ROOM + room), order * room + spot - ROOM, -64)
    set_keys(keys, (key,), weight_t[...])
    mix(keys, top, 0, top, 0, mix_ref, 0)

    taken = got.at[pl.ds(0, chips - 1)]
    pltpu.make_async_copy(taken, taken, recv_sem).wait()

    def cols_of(i, carry):
        cols = pl.ds(pl.multiple_of(i * COLS, COLS), COLS)
        out[:, cols] = total[:, cols] + weigh(got, mix_ref, cols)
        return carry
    lax.fori_loop(0, width // COLS, cols_of, 0)
    pltpu.make_async_copy(pack, pack, send_sem).wait()


def solution(mesh):
    n = mesh.shape["ep"]
    chips = n // 2

    def step(dispatched, w_gate, w_up, w_down, fill_count, slot_index, expert_id, gate_weight):
        sources, experts, cap, width = dispatched.shape
        ffn = w_gate.shape[2]
        tokens, top = slot_index.shape
        most = 2 * (HEADED * (cap - HEAD) + (experts - HEADED) * cap)
        cut = -(-ROOM // 16) * 8
        any_spec = pl.BlockSpec(memory_space=pl.ANY)
        vmem_spec = pl.BlockSpec(memory_space=pltpu.VMEM)
        smem_spec = pl.BlockSpec(memory_space=pltpu.SMEM)
        shape = jax.ShapeDtypeStruct
        vmem = pltpu.VMEM
        dma = pltpu.SemaphoreType.DMA
        fill_t, expert_t, slot_t, weight_t = fill_count.T, expert_id.T, slot_index.T, gate_weight.T
        own, other, table, branch, total = pl.pallas_call(
            functools.partial(main_kernel, n),
            name="main",
            out_shape=(
                shape((experts, chips, cap, width), BF16),
                shape((experts, chips, cap, width), BF16),
                shape((n, 8, 128), F32),
                shape((1, 1), I32),
                shape((tokens, width), F32),
            ),
            in_specs=[smem_spec] + [vmem_spec] * 4 + [any_spec] * 4,
            out_specs=(any_spec,) * 2 + (vmem_spec, smem_spec, vmem_spec),
            scratch_shapes=[
                vmem((2, 2, chips, cap, width), BF16),
                vmem((2, width, ffn), BF16),
                vmem((2, width, ffn), BF16),
                vmem((2, ffn, width), BF16),
                vmem((chips * cap, ffn), BF16),
                vmem((chips * cap, ffn), BF16),
                vmem((2 * experts, chips * cap, 128), F32),
                vmem((2, experts, chips, cap, width), BF16),
                vmem((experts, chips, cap, width), BF16),
                vmem((2, experts, chips, 8, width // 2), BF16),
                vmem((n * HEADED, 8, width // 2), BF16),
                vmem((8, 128), F32),
                vmem((n, 2 * experts * cap), I32),
                vmem((tokens, 128), F32),
                vmem((6 * tokens, n * HEADED * 8), BF16),
                vmem((3 * tokens, chips * cut), BF16),
                vmem((3 * tokens, chips * (ROOM - cut)), BF16),
                vmem((chips - 1, cut, width), BF16),
                vmem((chips - 1, ROOM - cut, width), BF16),
                vmem((chips, cut, width), BF16),
                vmem((chips, ROOM - cut, width), BF16),
                dma((3, 2)), dma((2, 2)), dma((2, ffn // COLS)), dma((experts,)), dma, dma((experts,)), dma((experts,)), dma((2,)), dma, dma, dma, dma((2,)), dma((2,)),
            ],
            compiler_params=pltpu.CompilerParams(collective_id=0, has_side_effects=True, vmem_limit_bytes=GRANT),
        )(fill_t, fill_t, expert_t, slot_t, weight_t, dispatched.reshape(chips, 2, experts, cap, width), w_gate, w_up, w_down)

        def more(room, index):
            result = pl.pallas_call(
                functools.partial(more_kernel, n, room),
                name="more%d" % room,
                out_shape=shape((tokens, width), F32),
                in_specs=[vmem_spec] * 5 + [any_spec] * 2,
                out_specs=vmem_spec,
                scratch_shapes=[
                    vmem((chips, 2, experts, cap, width), BF16),
                    vmem((chips - 1, room, width), BF16),
                    vmem((chips, room, width), BF16),
                    vmem((3 * tokens, chips * room), BF16),
                    vmem((n, 2 * experts * cap), I32),
                    vmem((tokens, 128), F32),
                    dma((chips, 2)), dma, dma,
                ],
                compiler_params=pltpu.CompilerParams(collective_id=1 + index, has_side_effects=True, vmem_limit_bytes=GRANT),
            )(table, expert_t, slot_t, weight_t, total, own, other)
            return result.astype(BF16)

        rooms = MORE + (most - ROOM,)
        return lax.switch(branch[0, 0], [lambda: total.astype(BF16)] + [functools.partial(more, r, i) for i, r in enumerate(rooms)])

    token_spec = P(("dp", "ep"))
    in_specs = (P("dp", "ep"), P("ep"), P("ep"), P("ep"), P("dp", "ep"), token_spec, token_spec, token_spec)
    return jax.shard_map(step, mesh=mesh, in_specs=in_specs, out_specs=token_spec, check_vma=False)
```

```python
import functools
import math

import jax
import jax.numpy as jnp
from jax import lax
from jax.experimental import pallas as pl
from jax.experimental.pallas import tpu as pltpu
from jax.sharding import PartitionSpec as P

MESH = pl.DeviceIdType.MESH
BF16, F32, I32 = jnp.bfloat16, jnp.float32, jnp.int32
HEAD = 4
HEADED = 3
COLS = 256
UNROLL = 3
CUT = 16
ROOM = 48
MORE = (8, 16, 24, 40)
GRANT = 64 * 1024 * 1024 - 65536
ORDER = ((2, 2), (2, 1), (2, 3), (1, 2), (3, 2), (2, 0), (0, 2), (1, 1), (3, 3), (1, 3), (3, 1), (1, 0), (3, 0), (0, 1), (0, 3))
STEP_X = sum(x << (2 * i) for i, (x, y) in enumerate(ORDER))
STEP_Y = sum(y << (2 * i) for i, (x, y) in enumerate(ORDER))


def step_to(chip, side, i):
    dx = lax.shift_right_logical(jnp.int32(STEP_X), 2 * i) & 3
    dy = lax.shift_right_logical(jnp.int32(STEP_Y), 2 * i) & 3
    return ((chip + dy * side) & (side * side - side)) + ((chip + dx) & (side - 1))


def iota(shape, dim):
    return lax.broadcasted_iota(I32, shape, dim)


def low(v, m):
    return v & (m - 1)


def high(v, m):
    return lax.shift_right_logical(v, m.bit_length() - 1)


def one(cond):
    return jnp.where(cond, 1.0, 0.0)


def needs(expert_t, slot_t, total, experts):
    tokens = expert_t.shape[1]
    hit = jnp.zeros((total, tokens), F32)
    for c in range(expert_t.shape[0]):
        hit = hit + one((iota((total, tokens), 0) == expert_t[c:c + 1]) & (slot_t[c:c + 1] >= 0))
    count = jnp.sum(hit, axis=1, keepdims=True)
    headed = low(iota((total, 1), 0), experts) < HEADED
    beyond = jnp.maximum(count - jnp.where(headed, float(HEAD), 0.0), 0.0)
    g, p = iota((total, total), 0), iota((total, total), 1)
    chip = high(g, 2 * experts) == high(p, 2 * experts)
    late_g, late_p = low(g, experts) == experts - 1, low(p, experts) == experts - 1
    first = one(chip & ~late_p & (late_g | (p < g))).astype(BF16)
    last = one(chip & late_p & late_g & (p < g)).astype(BF16)
    wide = jnp.broadcast_to(beyond, (total, 128)).astype(BF16)
    before = jnp.dot(first, wide, preferred_element_type=F32)
    late = low(iota((total, 128), 0), experts) == experts - 1
    before = jnp.where(late, jnp.maximum(before, float(CUT)), before) + jnp.dot(last, wide, preferred_element_type=F32)
    return beyond, before


def place_rows(table, me, core, n, experts, cap, place):
    lanes = 2 * experts * cap
    fills = jnp.concatenate([table[me, 0:experts], table[me + 1 - 2 * core, 0:experts], jnp.zeros((128 - 2 * experts, 128), F32)])
    fills = fills.T
    k, lane = iota((128, lanes), 0), iota((128, lanes), 1)
    early = low(iota((128, 128), 1), experts) < HEADED
    extra = jnp.maximum(fills - jnp.where(early, float(HEAD), 0.0), 0.0)
    k_lane = low(high(lane, cap), 2) * experts + high(lane, 2 * cap)
    rank_k = low(k + experts * core, 2 * experts)
    rank_l = low(k_lane + experts * core, 2 * experts)
    late_k, late_l = low(k, experts) == experts - 1, low(k_lane, experts) == experts - 1
    used = k < 2 * experts
    spread = one(k == k_lane).astype(BF16)
    first = one(used & ~late_k & (late_l | (rank_k < rank_l))).astype(BF16)
    last = one(used & late_k & late_l & (rank_k < rank_l)).astype(BF16)
    filled = jnp.dot(fills.astype(BF16), spread, preferred_element_type=F32)
    start = jnp.dot(extra.astype(BF16), first, preferred_element_type=F32)
    start = jnp.where(late_l, jnp.maximum(start, float(CUT)), start)
    start = start + jnp.dot(extra.astype(BF16), last, preferred_element_type=F32)
    slot = low(lane, cap)
    skip = jnp.where(low(k_lane, experts) < HEADED, HEAD, 0)
    spot = jnp.where((slot >= skip) & (slot.astype(F32) < filled), start.astype(I32) + slot - skip, -1)
    place[...] = spot[0:n]


def token_spots(expert, slot, before, chip, side, experts):
    total, tokens = before.shape[0], expert.shape[1]
    lead = []
    for c in range(expert.shape[0]):
        hit = iota((total, tokens), 0) == expert[c:c + 1]
        lead.append(jnp.sum(jnp.where(hit, before, 0.0), axis=0, keepdims=True))
    lead = jnp.concatenate(lead, axis=0).astype(I32)
    local = low(expert, experts)
    early = local < HEADED
    in_head = early & (slot >= 0) & (slot < HEAD)
    head_spot = jnp.where(in_head, (high(expert, experts) * HEADED + local) * 8 + slot, -64)
    home = high(expert, 2 * experts)
    order = jnp.full(expert.shape, side * side - 1, I32)
    for i, (dx, dy) in enumerate(ORDER):
        came = lax.rem(chip // side + side - dy, side) * side + lax.rem(lax.rem(chip, side) + side - dx, side)
        order = jnp.where(home == came, i, order)
    skip = jnp.where(early, HEAD, 0)
    return head_spot, order, jnp.where(slot >= skip, lead + slot - skip, -1)


def set_keys(keys, spots, weight):
    tokens = weight.shape[1]
    rows = [k.astype(F32) for k in spots] + [weight]
    rows.append(jnp.zeros((128 - len(rows) * weight.shape[0], tokens), F32))
    keys[...] = jnp.concatenate(rows).T


def mix(keys, top, first, weight, add, mix_ref, base):
    tokens = keys.shape[0]

    def tile(i, carry):
        lane = (iota((tokens, 128), 1) + (i * 128 - add)).astype(F32)
        w = jnp.zeros((tokens, 128), F32)
        for c in range(top):
            w = w + jnp.where(lane == keys[:, first + c:first + c + 1], keys[:, weight + c:weight + c + 1], 0.0)
        cols = pl.ds(pl.multiple_of(i * 128, 128), 128)
        for p, part in enumerate(split3(w)):
            mix_ref[pl.ds(base + p * tokens, tokens), cols] = part
        return carry
    lax.fori_loop(0, mix_ref.shape[1] // 128, tile, 0)


def fold(v, base, tokens):
    return v[base:base + tokens] + (v[base + tokens:base + 2 * tokens] + v[base + 2 * tokens:base + 3 * tokens])


def weigh(got, mix_ref, cols):
    rows = got.shape[0] * got.shape[1]
    v = jnp.dot(mix_ref[...], got[:, :, cols].reshape(rows, COLS), preferred_element_type=F32)
    return fold(v, 0, mix_ref.shape[0] // 3)


def main_kernel(n, fill_in, expert_in, slot_in, weight_in, x, w_gate, w_up, w_down, own, other, table, branch, total_out,
                fill, fill_v, expert_t, slot_t, weight_t, total, small_sem, out_sem, x_buf, gate_buf, up_buf, down_buf, hidden_a, hidden_b, mask, rows, theirs, head, head_in, note, place, keys,
                head_mix, mix_a, mix_b, pack_a, pack_b, got_a, got_b,
                load_sem, x_sem, piece_sem, own_sem, theirs_sem, pair_send, pair_recv, head_send, head_recv, note_send, note_recv, send_sem, recv_sem):
    me = lax.axis_index("ep")
    core = me & 1
    chip = lax.shift_right_logical(me, 1)
    chips = n // 2
    side = math.isqrt(chips)
    _, _, experts, cap, width = x.shape
    sources = n
    ffn = w_gate.shape[2]
    half = width // 2
    top, tokens = expert_t.shape
    cut = got_a.shape[1]
    rest = got_b.shape[1]
    hidden = (hidden_a, hidden_b)
    barrier = pltpu.get_barrier_semaphore()

    def load_x(e, h):
        return pltpu.make_async_copy(x.at[:, (core + 1 + h) & 1, e], x_buf.at[e & 1, h], x_sem.at[e & 1, h])

    def load_in(e):
        return (pltpu.make_async_copy(w_gate.at[e], gate_buf.at[e & 1], load_sem.at[0, e & 1]),
                pltpu.make_async_copy(w_up.at[e], up_buf.at[e & 1], load_sem.at[1, e & 1]))

    def load_down(e):
        return pltpu.make_async_copy(w_down.at[e], down_buf.at[e & 1], load_sem.at[2, e & 1])

    def load_piece(k):
        cols = pl.ds(k * COLS, COLS)
        return (pltpu.make_async_copy(w_gate.at[0, :, cols], gate_buf.at[0, :, cols], piece_sem.at[0, k]),
                pltpu.make_async_copy(w_up.at[0, :, cols], up_buf.at[0, :, cols], piece_sem.at[1, k]))

    pieces = ffn // COLS
    smalls = [pltpu.make_async_copy(a, b, small_sem.at[i]) for i, (a, b) in enumerate((
        (fill_in, fill), (fill_in, fill_v), (expert_in, expert_t), (slot_in, slot_t), (weight_in, weight_t)))]
    load_x(0, 0).start()
    for copy in load_piece(0):
        copy.start()
    for copy in smalls:
        copy.start()
    for k in range(1, pieces):
        for copy in load_piece(k):
            copy.start()
    load_down(0).start()
    load_x(0, 1).start()

    def greet(k, carry):
        pl.semaphore_signal(barrier, inc=1, device_id={"ep": (me + k) & (n - 1)}, device_id_type=MESH)
        return carry
    lax.fori_loop(1, n, greet, 0, unroll=8)

    for copy in smalls:
        copy.wait()
    beyond, before = needs(expert_t[...], slot_t[...], n * experts, experts)
    note[...] = jnp.zeros_like(note)
    note[0:experts, 0:sources] = fill_v[...].astype(F32)
    note[experts:experts + 1, :] = jnp.max(before + beyond, axis=0, keepdims=True)
    def set_mask(t, carry):
        for j in range(chips):
            full = fill[lax.shift_right_logical(t, 1), 2 * j + ((core + 1 + t) & 1)]
            mask[t, pl.ds(j * cap, cap), :] = one(iota((cap, 128), 0) < full)
        return carry
    lax.fori_loop(0, 2 * experts, set_mask, 0)

    def own_copy(e):
        return pltpu.make_async_copy(rows.at[1, e], own.at[e], own_sem.at[e])

    def pair_copy(e):
        return pltpu.make_async_remote_copy(
            src_ref=rows.at[0, e], dst_ref=theirs.at[e], send_sem=pair_send.at[e], recv_sem=pair_recv.at[e],
            device_id={"ep": me + 1 - 2 * core}, device_id_type=MESH)

    def up(e, h, k):
        cols = pl.ds(k * COLS, COLS)
        act = x_buf[e & 1, h].reshape(chips * cap, width)
        a = jnp.dot(act, gate_buf[e & 1, :, cols], preferred_element_type=F32)
        b = jnp.dot(act, up_buf[e & 1, :, cols], preferred_element_type=F32)
        hidden[h][:, cols] = (a * jax.nn.sigmoid(a) * b).astype(BF16)

    def down(e, h, k):
        live = jnp.concatenate([mask[2 * e + h]] * (COLS // 128), axis=1) > 0.5
        tops = []
        for part in range(2):
            cols = pl.ds(part * half + k * COLS, COLS)
            y = jnp.dot(hidden[h][...], down_buf[e & 1, :, cols], preferred_element_type=F32)
            y = jnp.where(live, y, 0.0)
            rows[h, e, :, :, cols] = y.astype(BF16).reshape(chips, cap, COLS)
            tops.append(y.reshape(chips, cap, COLS)[:, :8])
        first = iota((chips, 8, COLS), 1) < HEAD
        shifted = pltpu.roll(tops[1], HEAD, 1)
        head[h, e, :, :, pl.ds(k * COLS, COLS)] = jnp.where(first, tops[0], shifted).astype(BF16)

    outs = half // COLS

    def both(e_up, h_up, e_down, h_down):
        for k in range(max(pieces, outs)):
            if k < pieces:
                up(e_up, h_up, k)
            if k < outs:
                down(e_down, h_down, k)

    def push(e, h, j):
        pltpu.make_async_remote_copy(
            src_ref=head.at[h, e, j], dst_ref=head_in.at[me * HEADED + e], send_sem=head_send.at[h],
            recv_sem=head_recv, device_id={"ep": 2 * j + ((core + 1 + h) & 1)}, device_id_type=MESH).start()

    def push_all(e, h):
        def away(i, carry):
            push(e, h, step_to(chip, side, i))
            return carry
        lax.fori_loop(0, chips - 1, away, 0, unroll=True)

    def wait_notes(sem):
        noted = table.at[pl.ds(0, n - 1)]
        pltpu.make_async_copy(noted, noted, sem).wait()

    def chunk(p, j, count):
        first, size = ((0, cut), (cut, rest))[p]
        lanes = 2 * count * cap
        spots = place[pl.ds(2 * j + core, 1), :]
        pick = one(iota((size, lanes), 0) + first == spots[:, :lanes]).astype(BF16)
        near = rows[1, 0:count, pl.ds(j, 1)]
        far = theirs[0:count, pl.ds(j, 1)]
        source = jnp.concatenate([near, far], axis=1).reshape(lanes, width)
        return jnp.dot(pick, source, preferred_element_type=F32).astype(BF16)

    def send(p, i, j):
        return pltpu.make_async_remote_copy(
            src_ref=(pack_a, pack_b)[p].at[i], dst_ref=(got_a, got_b)[p].at[i], send_sem=send_sem.at[p],
            recv_sem=recv_sem.at[p], device_id={"ep": 2 * j + core}, device_id_type=MESH)

    def push_block(p, count):
        def one_chip(i, carry):
            j = step_to(chip, side, i)
            (pack_a, pack_b)[p][i] = chunk(p, j, count)
            send(p, i, j).start()
            return carry
        lax.fori_loop(0, chips - 1, one_chip, 0, unroll=UNROLL)
        (got_a, got_b)[p][chips - 1] = chunk(p, chip, count)

    load_x(0, 0).wait()
    for k in range(pieces):
        for copy in load_piece(k):
            copy.wait()
        if k == pieces - 1:
            for copy in load_in(1) + (load_x(1, 0), load_x(1, 1), load_down(1)):
                copy.start()
        up(0, 0, k)

    def expert(e, carry):
        @pl.when((e > 0) & (e + 1 < experts))
        def _():
            load_down(e + 1).start()

        load_x(e, 1).wait()
        load_down(e).wait()
        for k in range(outs):
            down(e, 0, k)

        @pl.when(e == 0)
        def _():
            pl.semaphore_wait(barrier, n - 1)

        pair_copy(e).start()

        @pl.when(e < HEADED)
        def _():
            push_all(e, 0)
            push(e, 0, chip)

        @pl.when(e == 0)
        def _():
            def tell(k, carry):
                pltpu.make_async_remote_copy(
                    src_ref=note, dst_ref=table.at[me], send_sem=note_send, recv_sem=note_recv,
                    device_id={"ep": (me + k) & (n - 1)}, device_id_type=MESH).start()
                return carry
            lax.fori_loop(1, n, tell, 0, unroll=8)
            table[me] = note[...]

        for k in range(pieces):
            up(e, 1, k)

        @pl.when(e + 2 < experts)
        def _():
            for copy in load_in(e + 2) + (load_x(e + 2, 0), load_x(e + 2, 1)):
                copy.start()

        for k in range(outs):
            down(e, 1, k)
        own_copy(e).start()

        @pl.when(e < HEADED)
        def _():
            push_all(e, 1)
            pltpu.make_async_copy(head.at[1, e, chip], head_in.at[me * HEADED + e], head_recv).start()

        @pl.when(e == experts - 2)
        def _():
            wait_notes(note_recv)
            place_rows(table, me, core, n, experts, cap, place)
            for done in range(experts - 1):
                pair_copy(done).wait_recv()
            push_block(0, experts - 1)

        @pl.when(e + 1 < experts)
        def _():
            load_x(e + 1, 0).wait()
            for copy in load_in(e + 1):
                copy.wait()
            for k in range(pieces):
                up(e + 1, 0, k)
        return carry
    lax.fori_loop(0, experts, expert, 0)

    wait_notes(note_send)
    pair_copy(experts - 1).wait_recv()
    push_block(1, experts)

    theirs_copy = pltpu.make_async_copy(theirs, other, theirs_sem)
    theirs_copy.start()
    most = jnp.max(jnp.max(table[...], axis=0)[experts:experts + 1, :])
    index = (most > float(cut + rest)).astype(I32)
    for more in MORE:
        index = index + (most > float(cut + rest + more)).astype(I32)
    branch[0, 0] = index

    _, before = needs(expert_t[...], slot_t[...], n * experts, experts)
    head_spot, order, spot = token_spots(expert_t[...], slot_t[...], before, chip, side, experts)
    key_a = jnp.where((spot >= 0) & (spot < cut), order * cut + spot, -64)
    key_b = jnp.where((spot >= cut) & (spot < cut + rest), order * rest + spot - cut, -64)
    set_keys(keys, (head_spot, key_a, key_b), weight_t[...])
    mix(keys, top, 0, 3 * top, 0, head_mix.at[pl.ds(0, 3 * tokens)], 0)
    mix(keys, top, 0, 3 * top, HEAD, head_mix.at[pl.ds(3 * tokens, 3 * tokens)], 0)
    mix(keys, top, top, 3 * top, 0, mix_a, 0)
    mix(keys, top, 2 * top, 3 * top, 0, mix_b, 0)
    pltpu.make_async_copy(head_in, head_in, head_recv).wait()

    def head_cols(i, carry):
        cols = pl.ds(pl.multiple_of(i * COLS, COLS), COLS)
        head_rows = head_in.shape[0] * head_in.shape[1]
        v = jnp.dot(head_mix[...], head_in[:, :, cols].reshape(head_rows, COLS), preferred_element_type=F32)
        total[:, cols] = fold(v, 0, tokens)
        total[:, pl.ds(pl.multiple_of(half + i * COLS, COLS), COLS)] = fold(v, 3 * tokens, tokens)
        return carry
    lax.fori_loop(0, half // COLS, head_cols, 0)

    for p, (got, mix_ref) in enumerate(((got_a, mix_a), (got_b, mix_b))):
        taken = got.at[pl.ds(0, chips - 1)]
        pltpu.make_async_copy(taken, taken, recv_sem.at[p]).wait()

        def some_cols(i, carry):
            cols = pl.ds(pl.multiple_of(i * COLS, COLS), COLS)
            total[:, cols] += weigh(got, mix_ref, cols)
            if p == 1:
                pltpu.make_async_copy(total.at[:, cols], total_out.at[:, cols], out_sem).start()
            return carry
        lax.fori_loop(0, width // COLS, some_cols, 0, unroll=p == 1)

    for p, sent in enumerate((pack_a, pack_b)):
        pltpu.make_async_copy(sent, sent, send_sem.at[p]).wait()
    pltpu.make_async_copy(total, total_out, out_sem).wait()
    for e in range(experts):
        own_copy(e).wait()
        pair_copy(e).wait_send()
    for h in range(2):
        sent = head.at[h, pl.ds(0, HEADED), pl.ds(0, chips - h)]
        pltpu.make_async_copy(sent, sent, head_send.at[h]).wait()
    theirs_copy.wait()


def split3(w):
    hi = jnp.minimum(w, 3.3895313892515355e38).astype(BF16)
    rest = w - hi.astype(F32)
    mid = rest.astype(BF16)
    low = (rest - mid.astype(F32)).astype(BF16)
    return hi, mid, low


def more_kernel(n, room, table, expert_t, slot_t, weight_t, total, own, other, out,
                src, pack, got, mix_ref, place, keys, load_sem, send_sem, recv_sem):
    me = lax.axis_index("ep")
    core = me & 1
    chip = lax.shift_right_logical(me, 1)
    chips = n // 2
    side = math.isqrt(chips)
    experts, _, cap, width = own.shape
    top, tokens = expert_t.shape
    barrier = pltpu.get_barrier_semaphore()

    def greet(i, carry):
        pl.semaphore_signal(barrier, inc=1, device_id={"ep": 2 * step_to(chip, side, i) + core}, device_id_type=MESH)
        return carry
    lax.fori_loop(0, chips - 1, greet, 0)

    def load(i, j):
        return (pltpu.make_async_copy(own.at[:, j], src.at[i, :, 0], load_sem.at[i, 0]),
                pltpu.make_async_copy(other.at[:, j], src.at[i, :, 1], load_sem.at[i, 1]))

    def load_to(i, carry):
        for copy in load(i, step_to(chip, side, i)):
            copy.start()
        return carry
    lax.fori_loop(0, chips - 1, load_to, 0)
    for copy in load(chips - 1, chip):
        copy.start()
    place_rows(table, me, core, n, experts, cap, place)

    def chunk(i, j):
        for copy in load(i, j):
            copy.wait()
        lanes = 2 * experts * cap
        pick = one(iota((room, lanes), 0) + ROOM == place[pl.ds(2 * j + core, 1), :]).astype(BF16)
        return jnp.dot(pick, src[i].reshape(lanes, width), preferred_element_type=F32).astype(BF16)

    def send(i, j):
        return pltpu.make_async_remote_copy(
            src_ref=pack.at[i], dst_ref=got.at[i], send_sem=send_sem, recv_sem=recv_sem,
            device_id={"ep": 2 * j + core}, device_id_type=MESH)

    pl.semaphore_wait(barrier, chips - 1)

    def push(i, carry):
        j = step_to(chip, side, i)
        pack[i] = chunk(i, j)
        send(i, j).start()
        return carry
    lax.fori_loop(0, chips - 1, push, 0)
    got[chips - 1] = chunk(chips - 1, chip)

    _, before = needs(expert_t[...], slot_t[...], n * experts, experts)
    _, order, spot = token_spots(expert_t[...], slot_t[...], before, chip, side, experts)
    key = jnp.where((spot >= ROOM) & (spot < ROOM + room), order * room + spot - ROOM, -64)
    set_keys(keys, (key,), weight_t[...])
    mix(keys, top, 0, top, 0, mix_ref, 0)

    taken = got.at[pl.ds(0, chips - 1)]
    pltpu.make_async_copy(taken, taken, recv_sem).wait()

    def cols_of(i, carry):
        cols = pl.ds(pl.multiple_of(i * COLS, COLS), COLS)
        out[:, cols] = total[:, cols] + weigh(got, mix_ref, cols)
        return carry
    lax.fori_loop(0, width // COLS, cols_of, 0)
    pltpu.make_async_copy(pack, pack, send_sem).wait()


def solution(mesh):
    n = mesh.shape["ep"]
    chips = n // 2

    def step(dispatched, w_gate, w_up, w_down, fill_count, slot_index, expert_id, gate_weight):
        sources, experts, cap, width = dispatched.shape
        ffn = w_gate.shape[2]
        tokens, top = slot_index.shape
        most = 2 * (HEADED * (cap - HEAD) + (experts - HEADED) * cap)
        cut = CUT
        any_spec = pl.BlockSpec(memory_space=pl.ANY)
        vmem_spec = pl.BlockSpec(memory_space=pltpu.VMEM)
        smem_spec = pl.BlockSpec(memory_space=pltpu.SMEM)
        shape = jax.ShapeDtypeStruct
        vmem = pltpu.VMEM
        dma = pltpu.SemaphoreType.DMA
        fill_t, expert_t, slot_t, weight_t = fill_count.T, expert_id.T, slot_index.T, gate_weight.T
        own, other, table, branch, total = pl.pallas_call(
            functools.partial(main_kernel, n),
            name="main",
            out_shape=(
                shape((experts, chips, cap, width), BF16),
                shape((experts, chips, cap, width), BF16),
                shape((n, 8, 128), F32),
                shape((1, 1), I32),
                shape((tokens, width), F32),
            ),
            in_specs=[any_spec] * 8,
            out_specs=(any_spec,) * 2 + (vmem_spec, smem_spec, any_spec),
            scratch_shapes=[
                pltpu.SMEM((experts, sources), I32),
                vmem((experts, sources), I32),
                vmem((top, tokens), I32),
                vmem((top, tokens), I32),
                vmem((top, tokens), F32),
                vmem((tokens, width), F32),
                dma((5,)), dma,
                vmem((2, 2, chips, cap, width), BF16),
                vmem((2, width, ffn), BF16),
                vmem((2, width, ffn), BF16),
                vmem((2, ffn, width), BF16),
                vmem((chips * cap, ffn), BF16),
                vmem((chips * cap, ffn), BF16),
                vmem((2 * experts, chips * cap, 128), F32),
                vmem((2, experts, chips, cap, width), BF16),
                vmem((experts, chips, cap, width), BF16),
                vmem((2, experts, chips, 8, width // 2), BF16),
                vmem((n * HEADED, 8, width // 2), BF16),
                vmem((8, 128), F32),
                vmem((n, 2 * experts * cap), I32),
                vmem((tokens, 128), F32),
                vmem((6 * tokens, n * HEADED * 8), BF16),
                vmem((3 * tokens, chips * cut), BF16),
                vmem((3 * tokens, chips * (ROOM - cut)), BF16),
                vmem((chips - 1, cut, width), BF16),
                vmem((chips - 1, ROOM - cut, width), BF16),
                vmem((chips, cut, width), BF16),
                vmem((chips, ROOM - cut, width), BF16),
                dma((3, 2)), dma((2, 2)), dma((2, ffn // COLS)), dma((experts,)), dma, dma((experts,)), dma((experts,)), dma((2,)), dma, dma, dma, dma((2,)), dma((2,)),
            ],
            compiler_params=pltpu.CompilerParams(collective_id=0, has_side_effects=True, vmem_limit_bytes=GRANT),
        )(fill_t, expert_t, slot_t, weight_t, dispatched.reshape(chips, 2, experts, cap, width), w_gate, w_up, w_down)

        def more(room, index):
            result = pl.pallas_call(
                functools.partial(more_kernel, n, room),
                name="more%d" % room,
                out_shape=shape((tokens, width), F32),
                in_specs=[vmem_spec] * 5 + [any_spec] * 2,
                out_specs=vmem_spec,
                scratch_shapes=[
                    vmem((chips, experts, 2, cap, width), BF16),
                    vmem((chips - 1, room, width), BF16),
                    vmem((chips, room, width), BF16),
                    vmem((3 * tokens, chips * room), BF16),
                    vmem((n, 2 * experts * cap), I32),
                    vmem((tokens, 128), F32),
                    dma((chips, 2)), dma, dma,
                ],
                compiler_params=pltpu.CompilerParams(collective_id=1 + index, has_side_effects=True, vmem_limit_bytes=GRANT),
            )(table, expert_t, slot_t, weight_t, total, own, other)
            return result.astype(BF16)

        rooms = MORE + (most - ROOM,)
        return lax.switch(branch[0, 0], [lambda: total.astype(BF16)] + [functools.partial(more, r, i) for i, r in enumerate(rooms)])

    token_spec = P(("dp", "ep"))
    in_specs = (P("dp", "ep"), P("ep"), P("ep"), P("ep"), P("dp", "ep"), token_spec, token_spec, token_spec)
    return jax.shard_map(step, mesh=mesh, in_specs=in_specs, out_specs=token_spec, check_vma=False)
```

```python
import functools
import math

import jax
import jax.numpy as jnp
from jax import lax
from jax.experimental import pallas as pl
from jax.experimental.pallas import tpu as pltpu
from jax.sharding import PartitionSpec as P

MESH = pl.DeviceIdType.MESH
BF16, F32, I32 = jnp.bfloat16, jnp.float32, jnp.int32
HEAD = 4
HEADED = 3
COLS = 256
UNROLL = 3
CUT = 16
ROOM = 48
MORE = (8, 16, 24, 40)
GRANT = 64 * 1024 * 1024 - 65536
ORDER = ((2, 2), (1, 2), (3, 2), (2, 1), (2, 3), (0, 2), (2, 0), (1, 1), (3, 3), (3, 1), (1, 3), (0, 1), (0, 3), (1, 0), (3, 0))
STEP_X = sum(x << (2 * i) for i, (x, y) in enumerate(ORDER))
STEP_Y = sum(y << (2 * i) for i, (x, y) in enumerate(ORDER))


def step_to(chip, side, i):
    dx = lax.shift_right_logical(jnp.int32(STEP_X), 2 * i) & 3
    dy = lax.shift_right_logical(jnp.int32(STEP_Y), 2 * i) & 3
    return ((chip + dy * side) & (side * side - side)) + ((chip + dx) & (side - 1))


def iota(shape, dim):
    return lax.broadcasted_iota(I32, shape, dim)


def low(v, m):
    return v & (m - 1)


def high(v, m):
    return lax.shift_right_logical(v, m.bit_length() - 1)


def one(cond):
    return jnp.where(cond, 1.0, 0.0)


def needs(expert_t, slot_t, total, experts):
    tokens = expert_t.shape[1]
    hit = jnp.zeros((total, tokens), F32)
    for c in range(expert_t.shape[0]):
        hit = hit + one((iota((total, tokens), 0) == expert_t[c:c + 1]) & (slot_t[c:c + 1] >= 0))
    count = jnp.sum(hit, axis=1, keepdims=True)
    headed = low(iota((total, 1), 0), experts) < HEADED
    beyond = jnp.maximum(count - jnp.where(headed, float(HEAD), 0.0), 0.0)
    g, p = iota((total, total), 0), iota((total, total), 1)
    chip = high(g, 2 * experts) == high(p, 2 * experts)
    late_g, late_p = low(g, experts) == experts - 1, low(p, experts) == experts - 1
    first = one(chip & ~late_p & (late_g | (p < g))).astype(BF16)
    last = one(chip & late_p & late_g & (p < g)).astype(BF16)
    wide = jnp.broadcast_to(beyond, (total, 128)).astype(BF16)
    before = jnp.dot(first, wide, preferred_element_type=F32)
    late = low(iota((total, 128), 0), experts) == experts - 1
    before = jnp.where(late, jnp.maximum(before, float(CUT)), before) + jnp.dot(last, wide, preferred_element_type=F32)
    return beyond, before


def place_rows(table, me, core, n, experts, cap, place):
    lanes = 2 * experts * cap
    fills = jnp.concatenate([table[me, 0:experts], table[me + 1 - 2 * core, 0:experts], jnp.zeros((128 - 2 * experts, 128), F32)])
    fills = fills.T
    k, lane = iota((128, lanes), 0), iota((128, lanes), 1)
    early = low(iota((128, 128), 1), experts) < HEADED
    extra = jnp.maximum(fills - jnp.where(early, float(HEAD), 0.0), 0.0)
    k_lane = low(high(lane, cap), 2) * experts + high(lane, 2 * cap)
    rank_k = low(k + experts * core, 2 * experts)
    rank_l = low(k_lane + experts * core, 2 * experts)
    late_k, late_l = low(k, experts) == experts - 1, low(k_lane, experts) == experts - 1
    used = k < 2 * experts
    spread = one(k == k_lane).astype(BF16)
    first = one(used & ~late_k & (late_l | (rank_k < rank_l))).astype(BF16)
    last = one(used & late_k & late_l & (rank_k < rank_l)).astype(BF16)
    filled = jnp.dot(fills.astype(BF16), spread, preferred_element_type=F32)
    start = jnp.dot(extra.astype(BF16), first, preferred_element_type=F32)
    start = jnp.where(late_l, jnp.maximum(start, float(CUT)), start)
    start = start + jnp.dot(extra.astype(BF16), last, preferred_element_type=F32)
    slot = low(lane, cap)
    skip = jnp.where(low(k_lane, experts) < HEADED, HEAD, 0)
    spot = jnp.where((slot >= skip) & (slot.astype(F32) < filled), start.astype(I32) + slot - skip, -1)
    place[...] = spot[0:n]


def token_spots(expert, slot, before, chip, side, experts):
    total, tokens = before.shape[0], expert.shape[1]
    lead = []
    for c in range(expert.shape[0]):
        hit = iota((total, tokens), 0) == expert[c:c + 1]
        lead.append(jnp.sum(jnp.where(hit, before, 0.0), axis=0, keepdims=True))
    lead = jnp.concatenate(lead, axis=0).astype(I32)
    local = low(expert, experts)
    early = local < HEADED
    in_head = early & (slot >= 0) & (slot < HEAD)
    head_spot = jnp.where(in_head, (high(expert, experts) * HEADED + local) * 8 + slot, -64)
    home = high(expert, 2 * experts)
    order = jnp.full(expert.shape, side * side - 1, I32)
    for i, (dx, dy) in enumerate(ORDER):
        came = lax.rem(chip // side + side - dy, side) * side + lax.rem(lax.rem(chip, side) + side - dx, side)
        order = jnp.where(home == came, i, order)
    skip = jnp.where(early, HEAD, 0)
    return head_spot, order, jnp.where(slot >= skip, lead + slot - skip, -1)


def set_keys(keys, spots, weight):
    tokens = weight.shape[1]
    rows = [k.astype(F32) for k in spots] + [weight]
    rows.append(jnp.zeros((128 - len(rows) * weight.shape[0], tokens), F32))
    keys[...] = jnp.concatenate(rows).T


def mix(keys, top, first, weight, add, mix_ref, base):
    tokens = keys.shape[0]

    def tile(i, carry):
        lane = (iota((tokens, 128), 1) + (i * 128 - add)).astype(F32)
        w = jnp.zeros((tokens, 128), F32)
        for c in range(top):
            w = w + jnp.where(lane == keys[:, first + c:first + c + 1], keys[:, weight + c:weight + c + 1], 0.0)
        cols = pl.ds(pl.multiple_of(i * 128, 128), 128)
        for p, part in enumerate(split3(w)):
            mix_ref[pl.ds(base + p * tokens, tokens), cols] = part
        return carry
    lax.fori_loop(0, mix_ref.shape[1] // 128, tile, 0)


def fold(v, base, tokens):
    return v[base:base + tokens] + (v[base + tokens:base + 2 * tokens] + v[base + 2 * tokens:base + 3 * tokens])


def weigh(got, mix_ref, cols):
    rows = got.shape[0] * got.shape[1]
    v = jnp.dot(mix_ref[...], got[:, :, cols].reshape(rows, COLS), preferred_element_type=F32)
    return fold(v, 0, mix_ref.shape[0] // 3)


def main_kernel(n, fill_in, expert_in, slot_in, weight_in, x, w_gate, w_up, w_down, own, other, table, branch, total_out,
                fill, fill_v, expert_t, slot_t, weight_t, total, small_sem, out_sem, x_buf, gate_buf, up_buf, down_buf, hidden_a, hidden_b, mask, rows, theirs, head, head_in, note, place, keys,
                head_mix, mix_a, mix_b, pack_a, pack_b, got_a, got_b,
                load_sem, x_sem, piece_sem, own_sem, theirs_sem, pair_send, pair_recv, head_send, head_recv, note_send, note_recv, send_sem, recv_sem):
    me = lax.axis_index("ep")
    core = me & 1
    chip = lax.shift_right_logical(me, 1)
    chips = n // 2
    side = math.isqrt(chips)
    _, _, experts, cap, width = x.shape
    sources = n
    ffn = w_gate.shape[2]
    half = width // 2
    top, tokens = expert_t.shape
    cut = got_a.shape[1]
    rest = got_b.shape[1]
    hidden = (hidden_a, hidden_b)
    barrier = pltpu.get_barrier_semaphore()

    def load_x(e, h):
        return pltpu.make_async_copy(x.at[:, (core + 1 + h) & 1, e], x_buf.at[e & 1, h], x_sem.at[e & 1, h])

    def load_in(e):
        return (pltpu.make_async_copy(w_gate.at[e], gate_buf.at[e & 1], load_sem.at[0, e & 1]),
                pltpu.make_async_copy(w_up.at[e], up_buf.at[e & 1], load_sem.at[1, e & 1]))

    def load_down(e):
        return pltpu.make_async_copy(w_down.at[e], down_buf.at[e & 1], load_sem.at[2, e & 1])

    def load_piece(k):
        cols = pl.ds(k * COLS, COLS)
        return (pltpu.make_async_copy(w_gate.at[0, :, cols], gate_buf.at[0, :, cols], piece_sem.at[0, k]),
                pltpu.make_async_copy(w_up.at[0, :, cols], up_buf.at[0, :, cols], piece_sem.at[1, k]))

    pieces = ffn // COLS
    smalls = [pltpu.make_async_copy(a, b, small_sem.at[i]) for i, (a, b) in enumerate((
        (fill_in, fill), (fill_in, fill_v), (expert_in, expert_t), (slot_in, slot_t), (weight_in, weight_t)))]
    load_x(0, 0).start()
    for copy in load_piece(0):
        copy.start()
    for copy in smalls:
        copy.start()
    for k in range(1, pieces):
        for copy in load_piece(k):
            copy.start()
    load_down(0).start()
    load_x(0, 1).start()

    def greet(k, carry):
        pl.semaphore_signal(barrier, inc=1, device_id={"ep": (me + k) & (n - 1)}, device_id_type=MESH)
        return carry
    lax.fori_loop(1, n, greet, 0, unroll=8)

    for copy in smalls:
        copy.wait()
    beyond, before = needs(expert_t[...], slot_t[...], n * experts, experts)
    note[...] = jnp.zeros_like(note)
    note[0:experts, 0:sources] = fill_v[...].astype(F32)
    note[experts:experts + 1, :] = jnp.max(before + beyond, axis=0, keepdims=True)
    def set_mask(t, carry):
        for j in range(chips):
            full = fill[lax.shift_right_logical(t, 1), 2 * j + ((core + 1 + t) & 1)]
            mask[t, pl.ds(j * cap, cap), :] = one(iota((cap, 128), 0) < full)
        return carry
    lax.fori_loop(0, 2 * experts, set_mask, 0)

    def own_copy(e):
        return pltpu.make_async_copy(rows.at[1, e], own.at[e], own_sem.at[e])

    def pair_copy(e):
        return pltpu.make_async_remote_copy(
            src_ref=rows.at[0, e], dst_ref=theirs.at[e], send_sem=pair_send.at[e], recv_sem=pair_recv.at[e],
            device_id={"ep": me + 1 - 2 * core}, device_id_type=MESH)

    def up(e, h, k):
        cols = pl.ds(k * COLS, COLS)
        act = x_buf[e & 1, h].reshape(chips * cap, width)
        a = jnp.dot(act, gate_buf[e & 1, :, cols], preferred_element_type=F32)
        b = jnp.dot(act, up_buf[e & 1, :, cols], preferred_element_type=F32)
        hidden[h][:, cols] = (a * jax.nn.sigmoid(a) * b).astype(BF16)

    def down(e, h, k):
        live = jnp.concatenate([mask[2 * e + h]] * (COLS // 128), axis=1) > 0.5
        tops = []
        for part in range(2):
            cols = pl.ds(part * half + k * COLS, COLS)
            y = jnp.dot(hidden[h][...], down_buf[e & 1, :, cols], preferred_element_type=F32)
            y = jnp.where(live, y, 0.0)
            rows[h, e, :, :, cols] = y.astype(BF16).reshape(chips, cap, COLS)
            tops.append(y.reshape(chips, cap, COLS)[:, :8])
        first = iota((chips, 8, COLS), 1) < HEAD
        shifted = pltpu.roll(tops[1], HEAD, 1)
        head[h, e, :, :, pl.ds(k * COLS, COLS)] = jnp.where(first, tops[0], shifted).astype(BF16)

    outs = half // COLS

    def both(e_up, h_up, e_down, h_down):
        for k in range(max(pieces, outs)):
            if k < pieces:
                up(e_up, h_up, k)
            if k < outs:
                down(e_down, h_down, k)

    def push(e, h, j):
        pltpu.make_async_remote_copy(
            src_ref=head.at[h, e, j], dst_ref=head_in.at[me * HEADED + e], send_sem=head_send.at[h],
            recv_sem=head_recv, device_id={"ep": 2 * j + ((core + 1 + h) & 1)}, device_id_type=MESH).start()

    def push_all(e, h):
        def away(i, carry):
            push(e, h, step_to(chip, side, i))
            return carry
        lax.fori_loop(0, chips - 1, away, 0, unroll=True)

    def wait_notes(sem):
        noted = table.at[pl.ds(0, n - 1)]
        pltpu.make_async_copy(noted, noted, sem).wait()

    def chunk(p, j, count):
        first, size = ((0, cut), (cut, rest))[p]
        lanes = 2 * count * cap
        spots = place[pl.ds(2 * j + core, 1), :]
        pick = one(iota((size, lanes), 0) + first == spots[:, :lanes]).astype(BF16)
        near = rows[1, 0:count, pl.ds(j, 1)]
        far = theirs[0:count, pl.ds(j, 1)]
        source = jnp.concatenate([near, far], axis=1).reshape(lanes, width)
        return jnp.dot(pick, source, preferred_element_type=F32).astype(BF16)

    def send(p, i, j):
        return pltpu.make_async_remote_copy(
            src_ref=(pack_a, pack_b)[p].at[i], dst_ref=(got_a, got_b)[p].at[i], send_sem=send_sem.at[p],
            recv_sem=recv_sem.at[p], device_id={"ep": 2 * j + core}, device_id_type=MESH)

    def push_block(p, count):
        def one_chip(i, carry):
            j = step_to(chip, side, i)
            (pack_a, pack_b)[p][i] = chunk(p, j, count)
            send(p, i, j).start()
            return carry
        lax.fori_loop(0, chips - 1, one_chip, 0, unroll=UNROLL)
        (got_a, got_b)[p][chips - 1] = chunk(p, chip, count)

    load_x(0, 0).wait()
    for k in range(pieces):
        for copy in load_piece(k):
            copy.wait()
        if k == pieces - 1:
            for copy in load_in(1) + (load_x(1, 0), load_x(1, 1), load_down(1)):
                copy.start()
        up(0, 0, k)

    def expert(e, carry):
        @pl.when((e > 0) & (e + 1 < experts))
        def _():
            load_down(e + 1).start()

        load_x(e, 1).wait()
        load_down(e).wait()
        for k in range(outs):
            down(e, 0, k)

        @pl.when(e == 0)
        def _():
            pl.semaphore_wait(barrier, n - 1)

        pair_copy(e).start()

        @pl.when(e < HEADED)
        def _():
            push_all(e, 0)
            push(e, 0, chip)

        @pl.when(e == 0)
        def _():
            def tell(k, carry):
                pltpu.make_async_remote_copy(
                    src_ref=note, dst_ref=table.at[me], send_sem=note_send, recv_sem=note_recv,
                    device_id={"ep": (me + k) & (n - 1)}, device_id_type=MESH).start()
                return carry
            lax.fori_loop(1, n, tell, 0, unroll=8)
            table[me] = note[...]

        for k in range(pieces):
            up(e, 1, k)

        @pl.when(e + 2 < experts)
        def _():
            for copy in load_in(e + 2) + (load_x(e + 2, 0), load_x(e + 2, 1)):
                copy.start()

        for k in range(outs):
            down(e, 1, k)
        own_copy(e).start()

        @pl.when(e < HEADED)
        def _():
            push_all(e, 1)
            pltpu.make_async_copy(head.at[1, e, chip], head_in.at[me * HEADED + e], head_recv).start()

        @pl.when(e == experts - 2)
        def _():
            wait_notes(note_recv)
            place_rows(table, me, core, n, experts, cap, place)
            for done in range(experts - 1):
                pair_copy(done).wait_recv()
            push_block(0, experts - 1)

        @pl.when(e + 1 < experts)
        def _():
            load_x(e + 1, 0).wait()
            for copy in load_in(e + 1):
                copy.wait()
            for k in range(pieces):
                up(e + 1, 0, k)
        return carry
    lax.fori_loop(0, experts, expert, 0)

    wait_notes(note_send)
    pair_copy(experts - 1).wait_recv()
    push_block(1, experts)

    theirs_copy = pltpu.make_async_copy(theirs, other, theirs_sem)
    theirs_copy.start()
    most = jnp.max(jnp.max(table[...], axis=0)[experts:experts + 1, :])
    index = (most > float(cut + rest)).astype(I32)
    for more in MORE:
        index = index + (most > float(cut + rest + more)).astype(I32)
    branch[0, 0] = index

    _, before = needs(expert_t[...], slot_t[...], n * experts, experts)
    head_spot, order, spot = token_spots(expert_t[...], slot_t[...], before, chip, side, experts)
    key_a = jnp.where((spot >= 0) & (spot < cut), order * cut + spot, -64)
    key_b = jnp.where((spot >= cut) & (spot < cut + rest), order * rest + spot - cut, -64)
    set_keys(keys, (head_spot, key_a, key_b), weight_t[...])
    mix(keys, top, 0, 3 * top, 0, head_mix.at[pl.ds(0, 3 * tokens)], 0)
    mix(keys, top, 0, 3 * top, HEAD, head_mix.at[pl.ds(3 * tokens, 3 * tokens)], 0)
    mix(keys, top, top, 3 * top, 0, mix_a, 0)
    mix(keys, top, 2 * top, 3 * top, 0, mix_b, 0)
    pltpu.make_async_copy(head_in, head_in, head_recv).wait()

    def head_cols(i, carry):
        cols = pl.ds(pl.multiple_of(i * COLS, COLS), COLS)
        head_rows = head_in.shape[0] * head_in.shape[1]
        v = jnp.dot(head_mix[...], head_in[:, :, cols].reshape(head_rows, COLS), preferred_element_type=F32)
        total[:, cols] = fold(v, 0, tokens)
        total[:, pl.ds(pl.multiple_of(half + i * COLS, COLS), COLS)] = fold(v, 3 * tokens, tokens)
        return carry
    lax.fori_loop(0, half // COLS, head_cols, 0)

    for p, (got, mix_ref) in enumerate(((got_a, mix_a), (got_b, mix_b))):
        taken = got.at[pl.ds(0, chips - 1)]
        pltpu.make_async_copy(taken, taken, recv_sem.at[p]).wait()

        def some_cols(i, carry):
            cols = pl.ds(pl.multiple_of(i * COLS, COLS), COLS)
            total[:, cols] += weigh(got, mix_ref, cols)
            if p == 1:
                pltpu.make_async_copy(total.at[:, cols], total_out.at[:, cols], out_sem).start()
            return carry
        lax.fori_loop(0, width // COLS, some_cols, 0, unroll=p == 1)

    for p, sent in enumerate((pack_a, pack_b)):
        pltpu.make_async_copy(sent, sent, send_sem.at[p]).wait()
    pltpu.make_async_copy(total, total_out, out_sem).wait()
    for e in range(experts):
        own_copy(e).wait()
        pair_copy(e).wait_send()
    for h in range(2):
        sent = head.at[h, pl.ds(0, HEADED), pl.ds(0, chips - h)]
        pltpu.make_async_copy(sent, sent, head_send.at[h]).wait()
    theirs_copy.wait()


def split3(w):
    hi = jnp.minimum(w, 3.3895313892515355e38).astype(BF16)
    rest = w - hi.astype(F32)
    mid = rest.astype(BF16)
    low = (rest - mid.astype(F32)).astype(BF16)
    return hi, mid, low


def more_kernel(n, room, table, expert_t, slot_t, weight_t, total, own, other, out,
                src, pack, got, mix_ref, place, keys, load_sem, send_sem, recv_sem):
    me = lax.axis_index("ep")
    core = me & 1
    chip = lax.shift_right_logical(me, 1)
    chips = n // 2
    side = math.isqrt(chips)
    experts, _, cap, width = own.shape
    top, tokens = expert_t.shape
    barrier = pltpu.get_barrier_semaphore()

    def greet(i, carry):
        pl.semaphore_signal(barrier, inc=1, device_id={"ep": 2 * step_to(chip, side, i) + core}, device_id_type=MESH)
        return carry
    lax.fori_loop(0, chips - 1, greet, 0)

    def load(i, j):
        return (pltpu.make_async_copy(own.at[:, j], src.at[i, :, 0], load_sem.at[i, 0]),
                pltpu.make_async_copy(other.at[:, j], src.at[i, :, 1], load_sem.at[i, 1]))

    def load_to(i, carry):
        for copy in load(i, step_to(chip, side, i)):
            copy.start()
        return carry
    lax.fori_loop(0, chips - 1, load_to, 0)
    for copy in load(chips - 1, chip):
        copy.start()
    place_rows(table, me, core, n, experts, cap, place)

    def chunk(i, j):
        for copy in load(i, j):
            copy.wait()
        lanes = 2 * experts * cap
        pick = one(iota((room, lanes), 0) + ROOM == place[pl.ds(2 * j + core, 1), :]).astype(BF16)
        return jnp.dot(pick, src[i].reshape(lanes, width), preferred_element_type=F32).astype(BF16)

    def send(i, j):
        return pltpu.make_async_remote_copy(
            src_ref=pack.at[i], dst_ref=got.at[i], send_sem=send_sem, recv_sem=recv_sem,
            device_id={"ep": 2 * j + core}, device_id_type=MESH)

    pl.semaphore_wait(barrier, chips - 1)

    def push(i, carry):
        j = step_to(chip, side, i)
        pack[i] = chunk(i, j)
        send(i, j).start()
        return carry
    lax.fori_loop(0, chips - 1, push, 0)
    got[chips - 1] = chunk(chips - 1, chip)

    _, before = needs(expert_t[...], slot_t[...], n * experts, experts)
    _, order, spot = token_spots(expert_t[...], slot_t[...], before, chip, side, experts)
    key = jnp.where((spot >= ROOM) & (spot < ROOM + room), order * room + spot - ROOM, -64)
    set_keys(keys, (key,), weight_t[...])
    mix(keys, top, 0, top, 0, mix_ref, 0)

    taken = got.at[pl.ds(0, chips - 1)]
    pltpu.make_async_copy(taken, taken, recv_sem).wait()

    def cols_of(i, carry):
        cols = pl.ds(pl.multiple_of(i * COLS, COLS), COLS)
        out[:, cols] = total[:, cols] + weigh(got, mix_ref, cols)
        return carry
    lax.fori_loop(0, width // COLS, cols_of, 0)
    pltpu.make_async_copy(pack, pack, send_sem).wait()


def solution(mesh):
    n = mesh.shape["ep"]
    chips = n // 2

    def step(dispatched, w_gate, w_up, w_down, fill_count, slot_index, expert_id, gate_weight):
        sources, experts, cap, width = dispatched.shape
        ffn = w_gate.shape[2]
        tokens, top = slot_index.shape
        most = 2 * (HEADED * (cap - HEAD) + (experts - HEADED) * cap)
        cut = CUT
        any_spec = pl.BlockSpec(memory_space=pl.ANY)
        vmem_spec = pl.BlockSpec(memory_space=pltpu.VMEM)
        smem_spec = pl.BlockSpec(memory_space=pltpu.SMEM)
        shape = jax.ShapeDtypeStruct
        vmem = pltpu.VMEM
        dma = pltpu.SemaphoreType.DMA
        fill_t, expert_t, slot_t, weight_t = fill_count.T, expert_id.T, slot_index.T, gate_weight.T
        own, other, table, branch, total = pl.pallas_call(
            functools.partial(main_kernel, n),
            name="main",
            out_shape=(
                shape((experts, chips, cap, width), BF16),
                shape((experts, chips, cap, width), BF16),
                shape((n, 8, 128), F32),
                shape((1, 1), I32),
                shape((tokens, width), F32),
            ),
            in_specs=[any_spec] * 8,
            out_specs=(any_spec,) * 2 + (vmem_spec, smem_spec, any_spec),
            scratch_shapes=[
                pltpu.SMEM((experts, sources), I32),
                vmem((experts, sources), I32),
                vmem((top, tokens), I32),
                vmem((top, tokens), I32),
                vmem((top, tokens), F32),
                vmem((tokens, width), F32),
                dma((5,)), dma,
                vmem((2, 2, chips, cap, width), BF16),
                vmem((2, width, ffn), BF16),
                vmem((2, width, ffn), BF16),
                vmem((2, ffn, width), BF16),
                vmem((chips * cap, ffn), BF16),
                vmem((chips * cap, ffn), BF16),
                vmem((2 * experts, chips * cap, 128), F32),
                vmem((2, experts, chips, cap, width), BF16),
                vmem((experts, chips, cap, width), BF16),
                vmem((2, experts, chips, 8, width // 2), BF16),
                vmem((n * HEADED, 8, width // 2), BF16),
                vmem((8, 128), F32),
                vmem((n, 2 * experts * cap), I32),
                vmem((tokens, 128), F32),
                vmem((6 * tokens, n * HEADED * 8), BF16),
                vmem((3 * tokens, chips * cut), BF16),
                vmem((3 * tokens, chips * (ROOM - cut)), BF16),
                vmem((chips - 1, cut, width), BF16),
                vmem((chips - 1, ROOM - cut, width), BF16),
                vmem((chips, cut, width), BF16),
                vmem((chips, ROOM - cut, width), BF16),
                dma((3, 2)), dma((2, 2)), dma((2, ffn // COLS)), dma((experts,)), dma, dma((experts,)), dma((experts,)), dma((2,)), dma, dma, dma, dma((2,)), dma((2,)),
            ],
            compiler_params=pltpu.CompilerParams(collective_id=0, has_side_effects=True, vmem_limit_bytes=GRANT),
        )(fill_t, expert_t, slot_t, weight_t, dispatched.reshape(chips, 2, experts, cap, width), w_gate, w_up, w_down)

        def more(room, index):
            result = pl.pallas_call(
                functools.partial(more_kernel, n, room),
                name="more%d" % room,
                out_shape=shape((tokens, width), F32),
                in_specs=[vmem_spec] * 5 + [any_spec] * 2,
                out_specs=vmem_spec,
                scratch_shapes=[
                    vmem((chips, experts, 2, cap, width), BF16),
                    vmem((chips - 1, room, width), BF16),
                    vmem((chips, room, width), BF16),
                    vmem((3 * tokens, chips * room), BF16),
                    vmem((n, 2 * experts * cap), I32),
                    vmem((tokens, 128), F32),
                    dma((chips, 2)), dma, dma,
                ],
                compiler_params=pltpu.CompilerParams(collective_id=1 + index, has_side_effects=True, vmem_limit_bytes=GRANT),
            )(table, expert_t, slot_t, weight_t, total, own, other)
            return result.astype(BF16)

        rooms = MORE + (most - ROOM,)
        return lax.switch(branch[0, 0], [lambda: total.astype(BF16)] + [functools.partial(more, r, i) for i, r in enumerate(rooms)])

    token_spec = P(("dp", "ep"))
    in_specs = (P("dp", "ep"), P("ep"), P("ep"), P("ep"), P("dp", "ep"), token_spec, token_spec, token_spec)
    return jax.shard_map(step, mesh=mesh, in_specs=in_specs, out_specs=token_spec, check_vma=False)
```
